512 devices in a mesh: path: 8 (over y_hi, x), mesh: 2 (over y_lo), grid: 32 (over z, core).
Axes of the slice: x: 4, y: 4 (y_hi: 2, y_lo: 2; y = y_hi * 2 + y_lo), z: 16, core: 2. Of those that a mesh axis runs over, the one named last changes fastest.
Arguments:
- path_bands: float32 [8, 16, 64, 64, 128], P('path', None, 'grid'), may hold values from -6 to 6
- occupied: float32 [2, 1, 64, 64, 128], P('mesh', None, 'grid', 'path'), may hold values from -6 to 6
- path_kpts: int32 [8, 3], P('path'), may hold values from 0 to 7
- mesh_kpts: int32 [2, 3], replicated, may hold values from 0 to 7
- mesh_shift: int32 [2, 3], replicated, may hold values from -1 to 1
Outputs:
- applied: float32 [8, 16, 64, 64, 128], P('path', 'mesh', 'grid')
- intersection: float32 [8, 2, 16, 16], P('path')
The draws below stay inside these ranges and needn't reach their ends.
All inputs are finite; a program needn't handle non-finite values.
Results may differ from the reference program's by a relative error of at most 0.0001.
Values sent between devices are 32-bit elements; how exact they have to be, the bound alone decides.
A program may use at most 64 MiB of HBM per device.

```python
import math
import jax
import jax.numpy as jnp
from jax import lax

NG = 64
NB = 16
NOCC = 1
KDIV = 8
NK = 8
NQ = 2


def plant(result, rng, least, largest):
    longest = result.shape.index(max(result.shape))
    spots = []
    for shift in (0, 1):
        where = [jax.random.randint(jax.random.fold_in(rng, axis), (), 0, length) for axis, length in enumerate(result.shape)]
        where[longest] = (where[longest] + shift) % result.shape[longest]
        spots.append(tuple(where))
    return result.at[spots[0]].set(least).at[spots[1]].set(largest)


def steps_of(stream_key, dims, shards, smallest, high):
    loudness, own = 1.0, jax.random.fold_in(stream_key, 6)
    for axis_at, parts in shards:
        steps = jnp.exp(jax.random.uniform(jax.random.fold_in(own, axis_at), (parts,), jnp.float32, smallest / len(shards), high / len(shards)))
        loudness = loudness * jnp.repeat(steps, dims[axis_at] // parts).reshape([-1 if axis == axis_at else 1 for axis in range(len(dims))])
    return loudness


def noise(rng, shape, spread, bound, split=(), kind=jnp.bfloat16):
    gain = steps_of(rng, shape, split, -0.22, 0.18) if split else 1.0
    entries = jax.random.normal(rng, shape, jnp.float32) * spread * gain
    return jnp.minimum(jnp.maximum(entries, -bound), bound).astype(kind)


def setup_inputs(seed: int = 0) -> dict:
    key_list = jax.random.split(jax.random.key(seed), 6)
    path_bands = noise(key_list[0], (NK, NB, NG, NG, 2 * NG), 1.0, 6.0, ((0, 8), (2, 32)), jnp.float32)
    occupied = noise(key_list[1], (NQ, NOCC, NG, NG, 2 * NG), 1.0, 6.0, ((0, 2), (2, 32), (3, 8)), jnp.float32)
    path_kpts = plant(jax.random.randint(key_list[2], (NK, 3), 0, KDIV), jax.random.fold_in(key_list[2], 1), 0, KDIV - 1).astype(jnp.int32)
    mesh_kpts = plant(jax.random.randint(key_list[3], (NQ, 3), 0, KDIV), jax.random.fold_in(key_list[3], 1), 0, KDIV - 1).astype(jnp.int32)
    mesh_shift = plant(jax.random.randint(key_list[4], (NQ, 3), -1, 2), jax.random.fold_in(key_list[4], 1), -1, 1).astype(jnp.int32)
    return {"path_bands": path_bands, "occupied": occupied, "path_kpts": path_kpts, "mesh_kpts": mesh_kpts, "mesh_shift": mesh_shift}


BOX_LENGTH = 42.7
SCREEN_SQ = 0.04
MIXING = 0.25
HIGHEST_PRECISION = lax.Precision.HIGHEST


def signed_frequencies(points):
    indices = jnp.arange(points, dtype=jnp.int32)
    return (indices + points // 2) % points - points // 2


def screened_coulomb(offset_frac):
    freqs = signed_frequencies(NG).astype(jnp.float32)
    squares = ((freqs + offset_frac[0]) ** 2)[:, None, None] + ((freqs + offset_frac[1]) ** 2)[None, :, None] + ((freqs + offset_frac[2]) ** 2)[None, None, :]
    return 4.0 * math.pi / ((2.0 * math.pi / BOX_LENGTH) ** 2 * squares + SCREEN_SQ)


def twist_phase(shift):
    coords = jnp.arange(NG, dtype=jnp.int32)
    product = (shift[0] * coords[:, None, None] + shift[1] * coords[None, :, None] + shift[2] * coords[None, None, :]) % NG
    angles = (2.0 * math.pi / NG) * product.astype(jnp.float32)
    return lax.complex(jnp.cos(angles), jnp.sin(angles))


def as_complex(values):
    return lax.complex(values[..., :NG], values[..., NG:])


def reference(path_bands, occupied, path_kpts, mesh_kpts, mesh_shift):
    rotated = [as_complex(occupied[mesh_point]) * twist_phase(mesh_shift[mesh_point]) for mesh_point in range(NQ)]

    def one_point(inputs):
        band_values, kpoint = inputs
        bands_complex = as_complex(band_values)
        applied = jnp.zeros_like(bands_complex)
        for mesh_point in range(NQ):
            offset_frac = (kpoint - mesh_kpts[mesh_point]).astype(jnp.float32) / KDIV
            kernel = screened_coulomb(offset_frac)
            orbitals = rotated[mesh_point]
            pair_density = jnp.conj(orbitals)[:, None] * bands_complex[None]
            potential = jnp.fft.ifftn(jnp.fft.fftn(pair_density, axes=(2, 3, 4)) * kernel, axes=(2, 3, 4))
            applied = applied - MIXING * jnp.sum(orbitals[:, None] * potential, axis=0)
        intersection = jnp.einsum("axyz,bxyz->ab", jnp.conj(bands_complex), applied, precision=HIGHEST_PRECISION) / NG ** 3
        return (jnp.concatenate([applied.real, applied.imag], -1), jnp.stack([intersection.real, intersection.imag]))

    applied_all, intersection_all = lax.map(one_point, (path_bands, path_kpts))
    return applied_all, intersection_all
```

```python
import functools
import math

import jax
import jax.numpy as jnp
import ml_dtypes
import numpy as np
from jax import lax
from jax.experimental import pallas as pl
from jax.experimental.pallas import tpu as pltpu
from jax.sharding import PartitionSpec as P

KDIV = 8
BOX_LENGTH = 42.7
SCREEN_SQ = 0.04
MIXING = 0.25
MESH = pl.DeviceIdType.MESH
F32 = jnp.float32
BF16 = jnp.bfloat16


def two_terms(table):
    high = table.astype(ml_dtypes.bfloat16)
    low = (table - high.astype(np.float64)).astype(ml_dtypes.bfloat16)
    return high, low


def tables(points):
    half = points // 2
    grid = np.arange(points)
    angles = 2.0 * np.pi / points * (grid[:, None] * grid[None, :] % points)
    cosine, sine = np.cos(angles), np.sin(angles)

    def left(cos_part, sin_part):
        high, low = two_terms(np.concatenate([cos_part, sin_part], 0))
        return np.concatenate([high, high, low, low], 1)

    def right(matrix):
        high, low = two_terms(matrix)
        upper = np.concatenate([high, low], 1)
        lower = np.concatenate([high, np.zeros_like(low)], 1)
        return np.concatenate([upper, lower], 0)

    parts = [slice(0, half), slice(half, points)]
    forward_y = np.stack([left(cosine[part], sine[part]) for part in parts])
    inverse_y = np.stack([left(cosine[:, part], sine[:, part]) for part in parts])
    along_x = left(cosine, sine)
    forward_z = right(np.block([[cosine, -sine], [sine, cosine]]))
    inverse_z = right(np.block([[cosine, sine], [-sine, cosine]]))
    return forward_y, along_x, inverse_y, forward_z, inverse_z


def split(values):
    high = values.astype(BF16)
    return high, (values - high.astype(F32)).astype(BF16)


def body(
    points, nz, npath, nbands,
    kp, km, shift, bands, occ, fy_h, lx_h, iy_h, fz_h, iz_h,
    applied, inter,
    band_full, occ_full, field, part, core_in, y_out, y_in, z_out, z_in, relay_in, mine,
    fy, lx, iy, fz, iz, base, pa, pb, pz, fin,
    loc, oz_s, oz_r, oh_s, oh_r, ox_s, ox_r, oc_s, oc_r,
    bz_s, bz_r, by_s, by_r, bc_s, bc_r, bl_s, bl_r,
    rc_s, rc_r, ry_s, ry_r, rz_s, rz_r, rr_s, rr_r, out_s,
    ia_s, ia_r, ib_s, ib_r, ic_s, ic_r,
):
    width = 2 * points
    half = points // 2
    nx = npath // 2
    rows = points // npath
    share = nbands // 2
    block = nbands // 2

    path = lax.axis_index("path")
    m = lax.axis_index("mesh")
    g = lax.axis_index("grid")
    z = lax.div(g, 2)
    c = lax.rem(g, 2)
    hi_y = lax.div(path, nx)
    at_x = lax.rem(path, nx)
    other_c, other_m = 1 - c, 1 - m
    core_peer = {"grid": 2 * z + other_c}
    y_peer = {"mesh": other_m}
    diag_peer = {"mesh": other_m, "grid": 2 * z + other_c}
    far_path = (1 - hi_y) * nx + at_x
    far_peer = {"path": far_path}

    def x_peer(j):
        return hi_y * nx + lax.rem(at_x + j, nx)

    def offset(i):
        return (nz // 2 - lax.div(i + 1, 2)) * (2 * lax.rem(i, 2) - 1)

    def target(i):
        return lax.rem(z + offset(i) + nz, nz)

    def source(i):
        return lax.rem(z - offset(i) + nz, nz)

    def ring(zz):
        return {"grid": 2 * zz + c}

    def remote(src, dst, send, recv, peer):
        return pltpu.make_async_remote_copy(
            src_ref=src, dst_ref=dst, send_sem=send, recv_sem=recv, device_id=peer, device_id_type=MESH
        )

    def plane(b, j):
        return pl.ds(pl.multiple_of((b * 2 + j) * points, points), points)

    def slab(b):
        return pl.ds(pl.multiple_of(b * points, points), points)

    def path_rows(p):
        return pl.ds(pl.multiple_of(p * rows, rows), rows)

    my_rows = path_rows(path)
    local = [
        pltpu.make_async_copy(occ.at[0, 0], occ_full.at[z, c, :, my_rows, :], loc.at[0]),
        pltpu.make_async_copy(bands.at[plane(z, 0)], band_full.at[z, c, 0], loc.at[1]),
        pltpu.make_async_copy(bands.at[plane(z, 1)], band_full.at[z, c, 1], loc.at[2]),
        pltpu.make_async_copy(fy_h.at[c], fy, loc.at[3]),
        pltpu.make_async_copy(lx_h, lx, loc.at[4]),
        pltpu.make_async_copy(iy_h.at[c], iy, loc.at[5]),
        pltpu.make_async_copy(fz_h, fz, loc.at[6]),
        pltpu.make_async_copy(iz_h, iz, loc.at[7]),
        pltpu.make_async_copy(bands, mine, loc.at[8]),
    ]
    for copy in local:
        copy.start()

    barrier = pltpu.get_barrier_semaphore()

    def greet(i, carry):
        pl.semaphore_signal(barrier, inc=1, device_id=ring(target(i)), device_id_type=MESH)
        return carry

    lax.fori_loop(0, nz - 1, greet, 0)
    for peer in (core_peer, y_peer, diag_peer, far_peer):
        pl.semaphore_signal(barrier, inc=1, device_id=peer, device_id_type=MESH)
    for j in range(1, nx):
        pl.semaphore_signal(barrier, inc=1, device_id={"path": x_peer(j)}, device_id_type=MESH)

    scale = (2.0 * math.pi / BOX_LENGTH) ** 2
    lane = lax.broadcasted_iota(jnp.int32, (points, width), 1)
    row = lax.broadcasted_iota(jnp.int32, (points, width), 0)

    def frequency(index, dim):
        shifted = (index - shift[m, dim] + half) & (points - 1)
        offset_frac = (kp[0, dim] - km[m, dim]).astype(F32) / KDIV
        return (shifted - half).astype(F32) + offset_frac

    freq_x = frequency(row, 0)
    freq_z = frequency(lane & (points - 1), 2)
    base[...] = scale * (freq_x * freq_x + freq_z * freq_z) + SCREEN_SQ

    pl.semaphore_wait(barrier, nz - 1 + 4 + nx - 1)

    def occ_z(i):
        return remote(
            occ.at[0, 0], occ_full.at[z, c, :, my_rows, :], oz_s.at[i], oz_r.at[i], ring(target(i))
        )

    def occ_z_in(i):
        spot = occ_full.at[source(i), c, :, my_rows, :]
        return remote(spot, spot, oz_s.at[i], oz_r.at[i], ring(source(i)))

    def band_z(i):
        dz = target(i)
        return remote(
            bands.at[plane(dz, m)], band_full.at[z, c, m], bz_s.at[i], bz_r.at[i], ring(dz)
        )

    def band_z_in(i):
        spot = band_full.at[source(i), c, m]
        return remote(spot, spot, bz_s.at[i], bz_r.at[i], ring(source(i)))

    def each(count, action):
        def step(i, carry):
            action(i)
            return carry

        lax.fori_loop(0, count, step, 0)

    each(nz - 1, lambda i: occ_z(i).start())
    each(nz - 1, lambda i: band_z(i).start())
    for copy in local[:3]:
        copy.wait()

    def band_own(to_mine):
        spot = band_full.at[z, other_c if to_mine else c]
        return remote(spot, spot, bl_s.at[0], bl_r.at[0], core_peer)

    band_own(False).start()

    def column(cc, p):
        return occ_full.at[:, cc, :, path_rows(p), :]

    def occ_far(p):
        return remote(column(c, p), column(c, p), oh_s.at[0], oh_r.at[0], far_peer)

    def occ_x(j, which, p):
        spot = column(c, p)
        return remote(
            spot, spot, ox_s.at[which, j], ox_r.at[which, j], {"path": x_peer(j)}
        )

    each(nz - 1, lambda i: occ_z_in(i).wait_recv())
    occ_far(path).start()
    for j in range(1, nx):
        occ_x(j, 0, path).start()

    def band_y(i, j):
        spot = band_full.at[source(i), c, j]
        return remote(spot, spot, by_s.at[i], by_r.at[i], y_peer)

    def band_core(i, cc, j, which):
        spot = band_full.at[source(i), cc, j]
        return remote(spot, spot, bc_s.at[which, i], bc_r.at[which, i], core_peer)

    def late(i):
        band_y(i, other_m).wait_recv()
        band_core(i, c, other_m, 1).start()

    def forward(i):
        band_z_in(i).wait_recv()
        band_y(i, m).start()
        band_core(i, c, m, 0).start()
        pl.when(i > 0)(lambda: late(i - 1))

    middle = nz // 2 - 1 if nz > 2 else 0
    each(middle, forward)
    occ_far(far_path).wait_recv()
    for j in range(1, nx):
        occ_x(j, 1, far_path).start()
    lax.fori_loop(middle, nz - 1, lambda i, carry: (forward(i), carry)[1], 0)
    late(nz - 2)
    for j in range(1, nx):
        near = hi_y * nx + lax.rem(at_x - j + nx, nx)
        distant = (1 - hi_y) * nx + lax.rem(at_x - j + nx, nx)
        occ_x(j, 0, near).wait_recv()
        occ_x(j, 1, distant).wait_recv()

    def occ_core(cc):
        spot = occ_full.at[:, cc]
        return remote(spot, spot, oc_s.at[0], oc_r.at[0], core_peer)

    occ_core(c).start()
    for copy in local[3:]:
        copy.wait()
    occ_core(other_c).wait_recv()

    lanes = lax.broadcasted_iota(jnp.int32, (1, width), 1)
    first = lanes < points

    def swap(values):
        return pltpu.roll(values, points, 1)

    def turned(values):
        moved = swap(values)
        return jnp.where(first, moved, -moved)

    def factors(values):
        moved = swap(values)
        return jnp.where(first, values, moved), jnp.where(first, moved, -values)

    def contract(matrix, tiles):
        stacked = jnp.concatenate(tiles, 1) if len(tiles) > 1 else tiles[0]
        high, low = split(stacked)
        right = jnp.concatenate([high, low, high, low], 0)
        out = jnp.dot(matrix, right, preferred_element_type=F32)
        count = out.shape[0] // 2
        return [
            (out[:count, t * width : (t + 1) * width], out[count:, t * width : (t + 1) * width])
            for t in range(len(tiles))
        ]

    def forward_sum(pair):
        return pair[0] + turned(pair[1])

    def inverse_sum(pair):
        return pair[0] - turned(pair[1])

    def along_z(matrix, values):
        high, low = split(values)
        out = jnp.dot(jnp.concatenate([high, low], 1), matrix, preferred_element_type=F32)
        return out[:, :width] + out[:, width:]

    def transform(zz):
        tiles = []
        for cc in range(2):
            for j in range(2):
                band = band_full[zz, cc, j]
                even, odd = factors(occ_full[zz, cc, j])
                tiles.append(even * band + odd * swap(band))
        summed = [forward_sum(pair) for pair in contract(fy[...], tiles)]
        spot = pl.ds(pl.multiple_of(zz * 4 * half, 4 * half), 4 * half)
        field[spot, :] = along_z(fz[...], jnp.concatenate(summed, 0))

    remote_own = band_own(True)
    remote_own.wait_recv()
    transform(z)

    def first_phase(i):
        band_core(i, other_c, m, 0).wait_recv()
        band_core(i, other_c, other_m, 1).wait_recv()
        transform(source(i))

    each(nz - 1, first_phase)

    batch = min(4, half)

    def second_phase(t):
        spots, tiles, kernels = [], [], []
        for k in range(batch):
            gy = t * batch + k
            spots.append(pl.ds(gy, points, stride=half))
            tiles.append(field[spots[k], :])
            freq_y = frequency(c * half + gy, 1)
            kernels.append(
                (-MIXING * 4.0 * math.pi / float(points**3)) / (base[...] + scale * (freq_y * freq_y))
            )
        spectra = [
            forward_sum(pair) * kernel for pair, kernel in zip(contract(lx[...], tiles), kernels)
        ]
        for k, pair in enumerate(contract(lx[...], spectra)):
            field[spots[k], :] = inverse_sum(pair)

    each(half // batch, second_phase)

    def restore(i):
        zz = target(i)
        spot = pl.ds(pl.multiple_of(zz * 4 * half, 4 * half), 4 * half)
        values = along_z(iz[...], field[spot, :])
        tiles = [values[t * half : (t + 1) * half] for t in range(4)]
        for t, pair in enumerate(contract(iy[...], tiles)):
            potential = inverse_sum(pair)
            even, odd = factors(occ_full[zz, t // 2, t % 2])
            part[i, t // 2, t % 2] = even * potential - odd * swap(potential)

    def give_core(i):
        return remote(part.at[i, other_c], core_in.at[i], rc_s.at[i], rc_r.at[i], core_peer)

    def give_y(i):
        return remote(y_out.at[i], y_in.at[i], ry_s.at[i], ry_r.at[i], y_peer)

    def give_z(i):
        return remote(z_out.at[i], z_in.at[slab(z)], rz_s.at[i], rz_r.at[i], ring(target(i)))

    def give_z_in(i):
        spot = z_in.at[slab(source(i))]
        return remote(spot, spot, rz_s.at[i], rz_r.at[i], ring(source(i)))

    def over_cores(i):
        give_core(i).wait_recv()
        y_out[i] = part[i, c, other_m] + core_in[i, other_m]
        z_out[i] = part[i, c, m] + core_in[i, m]

    def over_mesh(i):
        give_y(i).wait_recv()
        total = z_out[i] + y_in[i]
        z_out[i] = total
        pl.when(i == nz - 1)(lambda: keep(total))

    def keep(total):
        z_in[slab(z), :] = total

    lag_core, lag_mesh = 2, 5

    def third_phase(i):
        def at(step, low, high, action):
            pl.when((step >= low) & (step < high))(lambda: action(step))

        at(i - 1, 0, nz, lambda s: give_core(s).start())
        at(i - lag_core - 1, 0, nz, lambda s: give_y(s).start())
        at(i - lag_mesh - 1, 0, nz - 1, lambda s: give_z(s).start())
        at(i, 0, nz, restore)
        at(i - lag_core, 0, nz, over_cores)
        at(i - lag_mesh, 0, nz, over_mesh)

    each(nz + lag_mesh + 1, third_phase)

    def relay(b):
        k = lax.rem(b, share)
        return remote(z_in.at[slab(b)], relay_in.at[slab(k)], rr_s.at[k], rr_r.at[k], y_peer)

    def store(k, own):
        src = z_in.at[slab(m * share + k)] if own else relay_in.at[slab(k)]
        j = m if own else other_m
        return pltpu.make_async_copy(src, applied.at[plane(k, j)], out_s.at[0 if own else 1, k])

    def settle(b):
        owner = lax.div(b, share)
        pl.when(owner == m)(lambda: store(lax.rem(b, share), True).start())
        pl.when(owner != m)(lambda: relay(b).start())

    settle(z)

    def arrive(i):
        give_z_in(i).wait_recv()
        settle(source(i))

    each(nz - 1, arrive)

    def relayed(k):
        relay(other_m * share + k).wait_recv()
        store(k, False).start()

    each(share, relayed)

    chunk = min(16, points)

    def overlap(j, ref, start, total):
        def step(t, total):
            a_tiles, b_tiles = [], []
            for k in range(chunk):
                y = t * chunk + k
                a_tiles.append(mine[pl.ds(j * points + y, nbands, stride=2 * points), :])
                b_tiles.append(ref[pl.ds(start + y, share, stride=points), :])
            a_real = jnp.concatenate(a_tiles, 1)
            a_imag = jnp.concatenate([-turned(tile) for tile in a_tiles], 1)
            b_all = jnp.concatenate(b_tiles, 1)
            zero = jnp.zeros_like(b_all)
            b_all = jnp.concatenate(
                [jnp.where(m == 0, b_all, zero), jnp.where(m == 0, zero, b_all)], 0
            )
            a_high, a_low = split(jnp.concatenate([a_real, a_imag], 0))
            b_high, b_low = split(b_all)
            return total + lax.dot_general(
                jnp.concatenate([a_high, a_low, a_high], 1),
                jnp.concatenate([b_high, b_high, b_low], 1),
                (((1,), (1,)), ((), ())),
                preferred_element_type=F32,
            )

        return lax.fori_loop(0, points // chunk, step, total)

    total = jnp.zeros((2 * nbands, nbands), F32)
    total = overlap(m, z_in, m * share * points, total)
    total = overlap(other_m, relay_in, 0, total)
    pa[...] = jnp.zeros_like(pa)
    total = total * (1.0 / float(points**3))
    for k in range(4):
        pa[k, :, :nbands] = total[k * block : (k + 1) * block]

    quarter = 2 * m + c
    peers = [
        (core_peer, 2 * m + other_c),
        (y_peer, 2 * other_m + c),
        (diag_peer, 2 * other_m + other_c),
    ]

    def gather_pair(k):
        return remote(pa.at[peers[k][1]], pb.at[k], ia_s.at[k], ia_r.at[k], peers[k][0])

    for k in range(3):
        gather_pair(k).start()
    for k in range(3):
        gather_pair(k).wait_recv()
    pz[z] = (pa[quarter] + pb[0]) + (pb[1] + pb[2])

    def sum_z(i):
        return remote(pz.at[z], pz.at[z], ib_s.at[i], ib_r.at[i], ring(target(i)))

    def sum_z_in(i):
        spot = pz.at[source(i)]
        return remote(spot, spot, ib_s.at[i], ib_r.at[i], ring(source(i)))

    each(nz - 1, lambda i: sum_z(i).start())
    each(nz - 1, lambda i: sum_z_in(i).wait_recv())
    whole = pz[0]
    for k in range(1, nz):
        whole = whole + pz[k]
    fin[quarter] = whole

    def spread(k, into):
        spot = fin.at[into]
        return remote(spot, spot, ic_s.at[k], ic_r.at[k], peers[k][0])

    for k in range(3):
        spread(k, quarter).start()
    for k in range(3):
        spread(k, peers[k][1]).wait_recv()
    for k in range(4):
        inter[k * block : (k + 1) * block, :] = fin[k, :, :nbands]

    each(nz - 1, lambda i: occ_z(i).wait_send())
    each(nz - 1, lambda i: band_z(i).wait_send())
    band_own(False).wait_send()
    occ_far(path).wait_send()
    for j in range(1, nx):
        occ_x(j, 0, path).wait_send()
        occ_x(j, 1, far_path).wait_send()
    occ_core(c).wait_send()
    each(nz - 1, lambda i: band_y(i, m).wait_send())
    each(nz - 1, lambda i: band_core(i, c, m, 0).wait_send())
    each(nz - 1, lambda i: band_core(i, c, other_m, 1).wait_send())
    each(nz, lambda i: give_core(i).wait_send())
    each(nz, lambda i: give_y(i).wait_send())
    each(nz - 1, lambda i: give_z(i).wait_send())
    each(share, lambda k: relay(other_m * share + k).wait_send())
    each(share, lambda k: store(k, True).wait())
    each(share, lambda k: store(k, False).wait())
    for k in range(3):
        gather_pair(k).wait_send()
        spread(k, quarter).wait_send()
    each(nz - 1, lambda i: sum_z(i).wait_send())


def per_device(path_bands, occupied, path_kpts, mesh_kpts, mesh_shift):
    nbands, planes, points, width = path_bands.shape[1:]
    npath = lax.axis_size("path")
    nz = lax.axis_size("grid") // 2
    assert planes == 2 and nz == nbands and lax.axis_size("mesh") == 2
    half = points // 2
    share = nbands // 2
    forward_y, along_x, inverse_y, forward_z, inverse_z = tables(points)
    smem = pl.BlockSpec(memory_space=pltpu.SMEM)
    anywhere = pl.BlockSpec(memory_space=pl.ANY)
    vmem = lambda *shape: pltpu.VMEM(shape, F32)
    table = lambda array: pltpu.VMEM(array.shape, BF16)
    dma = lambda *shape: pltpu.SemaphoreType.DMA(shape)
    block = 2 * nbands // 4
    pairs = lambda *shape: [dma(*shape), dma(*shape)]
    scratch = [
        vmem(nz, 2, 2, points, width),
        vmem(nz, 2, 2, points, width),
        vmem(points * half, width),
        vmem(nz, 2, 2, points, width),
        vmem(nz, 2, points, width),
        vmem(nz, points, width),
        vmem(nz, points, width),
        vmem(nz, points, width),
        vmem(nbands * points, width),
        vmem(share * points, width),
        vmem(nbands * 2 * points, width),
        table(forward_y[0]),
        table(along_x),
        table(inverse_y[0]),
        table(forward_z),
        table(inverse_z),
        vmem(points, width),
        vmem(4, block, 128),
        vmem(3, block, 128),
        vmem(nz, block, 128),
        vmem(4, block, 128),
        dma(9),
        *pairs(nz),
        *pairs(1),
        *pairs(2, max(npath // 2, 1)),
        *pairs(1),
        *pairs(nz),
        *pairs(nz),
        *pairs(2, nz),
        *pairs(1),
        *pairs(nz),
        *pairs(nz),
        *pairs(nz),
        *pairs(share),
        dma(2, share),
        *pairs(3),
        *pairs(nz),
        *pairs(3),
    ]
    applied, inter = pl.pallas_call(
        functools.partial(body, points, nz, npath, nbands),
        name="exchange",
        out_shape=(
            jax.ShapeDtypeStruct((share * 2 * points, width), F32),
            jax.ShapeDtypeStruct((2 * nbands, nbands), F32),
        ),
        in_specs=[smem] * 3 + [anywhere] * 7,
        out_specs=(anywhere, pl.BlockSpec(memory_space=pltpu.VMEM)),
        scratch_shapes=scratch,
        compiler_params=pltpu.CompilerParams(
            collective_id=0, has_side_effects=True, vmem_limit_bytes=40 << 20
        ),
    )(
        path_kpts,
        mesh_kpts,
        mesh_shift,
        path_bands.reshape(nbands * planes * points, width),
        occupied,
        jnp.asarray(forward_y),
        jnp.asarray(along_x),
        jnp.asarray(inverse_y),
        jnp.asarray(forward_z),
        jnp.asarray(inverse_z),
    )
    return (
        applied.reshape(1, share, planes, points, width),
        inter.reshape(1, 2, nbands, nbands),
    )


def solution(mesh):
    return jax.shard_map(
        per_device,
        mesh=mesh,
        in_specs=(
            P("path", None, "grid", None, None),
            P("mesh", None, "grid", "path", None),
            P("path", None),
            P(),
            P(),
        ),
        out_specs=(P("path", "mesh", "grid", None, None), P("path", None, None, None)),
        check_vma=False,
    )
```

```python
import functools
import math

import jax
import jax.numpy as jnp
import ml_dtypes
import numpy as np
from jax import lax
from jax.experimental import pallas as pl
from jax.experimental.pallas import tpu as pltpu
from jax.sharding import PartitionSpec as P

KDIV = 8
BOX_LENGTH = 42.7
SCREEN_SQ = 0.04
MIXING = 0.25
MESH = pl.DeviceIdType.MESH
F32 = jnp.float32
BF16 = jnp.bfloat16


def two_terms(table):
    high = table.astype(ml_dtypes.bfloat16)
    low = (table - high.astype(np.float64)).astype(ml_dtypes.bfloat16)
    return high, low


def tables(points):
    half = points // 2
    grid = np.arange(points)
    angles = 2.0 * np.pi / points * (grid[:, None] * grid[None, :] % points)
    cosine, sine = np.cos(angles), np.sin(angles)

    def left(cos_part, sin_part):
        high, low = two_terms(np.concatenate([cos_part, sin_part], 0))
        return np.concatenate([high, high, low, low], 1)

    def right(matrix):
        high, low = two_terms(matrix)
        upper = np.concatenate([high, low], 1)
        lower = np.concatenate([high, np.zeros_like(low)], 1)
        return np.concatenate([upper, lower], 0)

    parts = [slice(0, half), slice(half, points)]
    forward_y = np.stack([left(cosine[part], sine[part]) for part in parts])
    inverse_y = np.stack([left(cosine[:, part], sine[:, part]) for part in parts])
    along_x = left(cosine, sine)
    forward_z = right(np.block([[cosine, -sine], [sine, cosine]]))
    inverse_z = right(np.block([[cosine, sine], [-sine, cosine]]))
    return forward_y, along_x, inverse_y, forward_z, inverse_z


def split(values):
    high = values.astype(BF16)
    return high, (values - high.astype(F32)).astype(BF16)


def layout(points, nz):
    near_count = {16: 4}.get(nz, 2)
    return nz // near_count, near_count, points // 2 + 8


def body(
    points, nz, npath, nbands,
    kp_h, km_h, shift_h, bands, occ, fy_h, lx_h, iy_h, fz_h, iz_h,
    applied, inter,
    band_full, occ_full, field, part, core_in, y_out, y_in, z_out, z_in, relay_in, mine,
    fy, lx, iy, fz, iz, base, acc, pz, fin, kp, km, shift,
    loc, of_s, of_r, on_s, on_r, oh_s, oh_r, ox_s, ox_r, oc_s, oc_r,
    bz_s, bz_r, by_s, by_r, bc_s, bc_r, bl_s, bl_r,
    rc_s, rc_r, ry_s, ry_r, rz_s, rz_r, rr_s, rr_r, out_s,
    ib_s, ib_r, ic_s, ic_r,
):
    width = 2 * points
    half = points // 2
    nx = npath // 2
    rows = points // npath
    share = nbands // 2
    block = nbands // 2
    far_count, near_count, pitch = layout(points, nz)

    path = lax.axis_index("path")
    m = lax.axis_index("mesh")
    g = lax.axis_index("grid")
    z = lax.div(g, 2)
    c = lax.rem(g, 2)
    hi_y = lax.div(path, nx)
    at_x = lax.rem(path, nx)
    other_c, other_m = 1 - c, 1 - m
    core_peer = {"grid": 2 * z + other_c}
    y_peer = {"mesh": other_m}
    diag_peer = {"mesh": other_m, "grid": 2 * z + other_c}
    far_path = (1 - hi_y) * nx + at_x
    far_peer = {"path": far_path}

    def x_peer(j):
        return hi_y * nx + lax.rem(at_x + j, nx)

    def offset(i):
        return (lax.div(i, 2) + 1) * (1 - 2 * lax.rem(i, 2)) * jnp.where(i == nz - 1, 0, 1)

    def target(i):
        return lax.rem(z + offset(i) + nz, nz)

    def source(i):
        return lax.rem(z - offset(i) + nz, nz)

    def ring(zz):
        return {"grid": 2 * zz + c}

    def remote(src, dst, send, recv, peer):
        return pltpu.make_async_remote_copy(
            src_ref=src, dst_ref=dst, send_sem=send, recv_sem=recv, device_id=peer, device_id_type=MESH
        )

    def plane(b, j):
        return pl.ds(pl.multiple_of((b * 2 + j) * points, points), points)

    def slab(b):
        return pl.ds(pl.multiple_of(b * points, points), points)

    def path_rows(p):
        return pl.ds(pl.multiple_of(p * rows, rows), rows)

    my_rows = path_rows(path)
    far, near = lax.div(z, near_count), lax.rem(z, near_count)
    local = [
        pltpu.make_async_copy(occ.at[0, 0], occ_full.at[far, near, c, :, my_rows, :], loc.at[0]),
        pltpu.make_async_copy(bands.at[plane(z, 0)], band_full.at[z, c, 0], loc.at[1]),
        pltpu.make_async_copy(bands.at[plane(z, 1)], band_full.at[z, c, 1], loc.at[2]),
        pltpu.make_async_copy(fy_h.at[c], fy, loc.at[3]),
        pltpu.make_async_copy(lx_h, lx, loc.at[4]),
        pltpu.make_async_copy(iy_h.at[c], iy, loc.at[5]),
        pltpu.make_async_copy(fz_h, fz, loc.at[6]),
        pltpu.make_async_copy(iz_h, iz, loc.at[7]),
        pltpu.make_async_copy(kp_h, kp, loc.at[8]),
        pltpu.make_async_copy(km_h, km, loc.at[9]),
        pltpu.make_async_copy(shift_h, shift, loc.at[10]),
        pltpu.make_async_copy(bands, mine, loc.at[11]),
    ]
    for copy in local:
        copy.start()

    barrier = pltpu.get_barrier_semaphore()

    def greet(i, carry):
        pl.semaphore_signal(barrier, inc=1, device_id=ring(target(i)), device_id_type=MESH)
        return carry

    lax.fori_loop(0, nz - 1, greet, 0)
    for peer in (core_peer, y_peer, diag_peer, far_peer):
        pl.semaphore_signal(barrier, inc=1, device_id=peer, device_id_type=MESH)
    for j in range(1, nx):
        pl.semaphore_signal(barrier, inc=1, device_id={"path": x_peer(j)}, device_id_type=MESH)

    pl.semaphore_wait(barrier, nz - 1 + 4 + nx - 1)

    def each(low, high, action):
        def step(i, carry):
            action(i)
            return carry

        lax.fori_loop(low, high, step, 0)

    near_steps = [(1, -1, 2)[e] for e in range(near_count - 1)]

    def occ_far_z(k, back=False):
        at = lax.rem(far + (far_count - k if back else k), far_count)
        spot = occ_full.at[at if back else far, near, c, :, my_rows, :]
        src = spot if back else occ.at[0, 0]
        return remote(src, spot, of_s.at[k], of_r.at[k], ring(at * near_count + near))

    def occ_near_z(k, back=False):
        step = near_steps[k]
        zz = lax.rem(z + nz - step if back else z + nz + step, nz)
        spot = occ_full.at[:, lax.rem(zz, near_count) if back else near, c, :, my_rows, :]
        return remote(spot, spot, on_s.at[k], on_r.at[k], ring(zz))

    def band_z(i):
        dz = target(i)
        return remote(
            bands.at[plane(dz, m)], band_full.at[z, c, m], bz_s.at[i], bz_r.at[i], ring(dz)
        )

    def band_z_in(i):
        spot = band_full.at[source(i), c, m]
        return remote(spot, spot, bz_s.at[i], bz_r.at[i], ring(source(i)))

    def band_own(to_mine):
        spot = band_full.at[z, other_c if to_mine else c]
        return remote(spot, spot, bl_s.at[0], bl_r.at[0], core_peer)

    def column(cc, p):
        return occ_full.at[:, :, cc, :, path_rows(p), :]

    def occ_far(p):
        return remote(column(c, p), column(c, p), oh_s.at[0], oh_r.at[0], far_peer)

    def occ_x(j, which, p):
        spot = column(c, p)
        return remote(
            spot, spot, ox_s.at[which, j], ox_r.at[which, j], {"path": x_peer(j)}
        )

    def occ_core(cc, p):
        spot = column(cc, p)
        return remote(spot, spot, oc_s.at[p], oc_r.at[p], core_peer)

    def band_y(i, j):
        spot = band_full.at[source(i), c, j]
        return remote(spot, spot, by_s.at[i], by_r.at[i], y_peer)

    def band_core(i, cc, j, which):
        spot = band_full.at[source(i), cc, j]
        return remote(spot, spot, bc_s.at[which, i], bc_r.at[which, i], core_peer)

    def late(i):
        band_y(i, other_m).wait_recv()
        band_core(i, c, other_m, 1).start()

    def forward(i):
        band_z_in(i).wait_recv()
        band_y(i, m).start()
        band_core(i, c, m, 0).start()
        pl.when(i > 0)(lambda: late(i - 1))

    steps = nz - 1
    first_stop, second_stop, third_stop, fourth_stop = (
        (4, 8, 9, 10) if nz == 16 else (1, steps, steps, steps)
    )
    for k in range(1, far_count):
        occ_far_z(k).start()
    each(0, second_stop, lambda i: band_z(i).start())
    for copy in local[:3]:
        copy.wait()
    band_own(False).start()
    each(0, first_stop, forward)
    for k in range(1, far_count):
        occ_far_z(k, True).wait_recv()
    for k in range(near_count - 1):
        occ_near_z(k).start()
    each(second_stop, steps, lambda i: band_z(i).start())
    for copy in local[3:]:
        copy.wait()

    scale = (2.0 * math.pi / BOX_LENGTH) ** 2
    lane = lax.broadcasted_iota(jnp.int32, (points, width), 1)
    row = lax.broadcasted_iota(jnp.int32, (points, width), 0)

    def frequency(index, dim):
        shifted = (index - shift[m, dim] + half) & (points - 1)
        offset_frac = (kp[0, dim] - km[m, dim]).astype(F32) / KDIV
        return (shifted - half).astype(F32) + offset_frac

    freq_x = frequency(row, 0)
    freq_z = frequency(lane & (points - 1), 2)
    base[...] = scale * (freq_x * freq_x + freq_z * freq_z) + SCREEN_SQ

    for k in range(near_count - 1):
        occ_near_z(k, True).wait_recv()
    occ_far(path).start()
    for j in range(1, nx):
        occ_x(j, 0, path).start()
    occ_core(c, path).start()
    each(first_stop, third_stop, forward)
    occ_far(far_path).wait_recv()
    for j in range(1, nx):
        occ_x(j, 1, far_path).start()
    occ_core(c, far_path).start()
    each(third_stop, fourth_stop, forward)
    for which in range(2):
        for j in range(1, nx):
            side = hi_y if which == 0 else 1 - hi_y
            p = side * nx + lax.rem(at_x - j + nx, nx)
            occ_x(j, which, p).wait_recv()
            occ_core(c, p).start()
    each(0, npath, lambda p: occ_core(other_c, p).wait_recv())

    lanes = lax.broadcasted_iota(jnp.int32, (1, width), 1)
    first = lanes < points

    def swap(values):
        return pltpu.roll(values, points, 1)

    def turned(values):
        moved = swap(values)
        return jnp.where(first, moved, -moved)

    def factors(values):
        moved = swap(values)
        return jnp.where(first, values, moved), jnp.where(first, moved, -values)

    def contract(matrix, tiles):
        stacked = jnp.concatenate(tiles, 1) if len(tiles) > 1 else tiles[0]
        high, low = split(stacked)
        right = jnp.concatenate([high, low, high, low], 0)
        out = jnp.dot(matrix, right, preferred_element_type=F32)
        count = out.shape[0] // 2
        return [
            (out[:count, t * width : (t + 1) * width], out[count:, t * width : (t + 1) * width])
            for t in range(len(tiles))
        ]

    def forward_sum(pair):
        return pair[0] + turned(pair[1])

    def inverse_sum(pair):
        return pair[0] - turned(pair[1])

    def along_z(matrix, values):
        high, low = split(values)
        out = jnp.dot(jnp.concatenate([high, low], 1), matrix, preferred_element_type=F32)
        return out[:, :width] + out[:, width:]

    def orbital(zz, cc, j):
        return occ_full[lax.div(zz, near_count), lax.rem(zz, near_count), cc, j]

    def x_rows(zz, t):
        return pl.ds(pl.multiple_of((zz * 4 + t) * pitch, 8), half)

    def transform(zz):
        tiles = []
        for t in range(4):
            band = band_full[zz, t // 2, t % 2]
            even, odd = factors(orbital(zz, t // 2, t % 2))
            tiles.append(even * band + odd * swap(band))
        summed = [forward_sum(pair) for pair in contract(fy[...], tiles)]
        values = along_z(fz[...], jnp.concatenate(summed, 0))
        for t in range(4):
            field[x_rows(zz, t), :] = values[t * half : (t + 1) * half]

    def first_phase(t):
        step = fourth_stop + lax.div(t, 3)
        turn = lax.rem(t, 3) == 0
        pl.when(turn & (step < steps))(lambda: forward(step))
        pl.when(turn & (step == steps))(lambda: late(steps - 1))

        def fetched():
            band_core(t - 1, other_c, m, 0).wait_recv()
            band_core(t - 1, other_c, other_m, 1).wait_recv()

        pl.when(t > 0)(fetched)
        pl.when(t == 0)(lambda: band_own(True).wait_recv())
        transform(source(jnp.where(t == 0, nz - 1, t - 1)))

    each(0, nz, first_phase)

    batch = min(4, half)

    def second_phase(t):
        spots, tiles, kernels = [], [], []
        for k in range(batch):
            gy = t * batch + k
            spots.append(pl.ds(gy, points, stride=pitch))
            tiles.append(field[spots[k], :])
            freq_y = frequency(c * half + gy, 1)
            kernels.append(
                (-MIXING * 4.0 * math.pi / float(points**3)) / (base[...] + scale * (freq_y * freq_y))
            )
        spectra = [
            forward_sum(pair) * kernel for pair, kernel in zip(contract(lx[...], tiles), kernels)
        ]
        for k, pair in enumerate(contract(lx[...], spectra)):
            field[spots[k], :] = inverse_sum(pair)

    each(0, half // batch, second_phase)

    def restore(i):
        zz = target(i)
        values = along_z(
            iz[...], jnp.concatenate([field[x_rows(zz, t), :] for t in range(4)], 0)
        )
        tiles = [values[t * half : (t + 1) * half] for t in range(4)]
        for t, pair in enumerate(contract(iy[...], tiles)):
            potential = inverse_sum(pair)
            even, odd = factors(orbital(zz, t // 2, t % 2))
            part[i, t // 2, t % 2] = even * potential - odd * swap(potential)

    def give_core(i):
        return remote(part.at[i, other_c], core_in.at[i], rc_s.at[i], rc_r.at[i], core_peer)

    def give_y(i):
        return remote(y_out.at[i], y_in.at[i], ry_s.at[i], ry_r.at[i], y_peer)

    def give_z(i):
        return remote(z_out.at[i], z_in.at[slab(z)], rz_s.at[i], rz_r.at[i], ring(target(i)))

    def give_z_in(i):
        spot = z_in.at[slab(source(i))]
        return remote(spot, spot, rz_s.at[i], rz_r.at[i], ring(source(i)))

    def over_cores(i):
        give_core(i).wait_recv()
        y_out[i] = part[i, c, other_m] + core_in[i, other_m]
        z_out[i] = part[i, c, m] + core_in[i, m]

    def over_mesh(i):
        give_y(i).wait_recv()
        total = z_out[i] + y_in[i]
        z_out[i] = total
        pl.when(i == nz - 1)(lambda: keep(total))

    def keep(total):
        z_in[slab(z), :] = total

    lag_core, lag_mesh = 2, 5

    def third_phase(i):
        def at(step, low, high, action):
            pl.when((step >= low) & (step < high))(lambda: action(step))

        at(i - 1, 0, nz, lambda s: give_core(s).start())
        at(i - lag_core - 1, 0, nz, lambda s: give_y(s).start())
        at(i - lag_mesh - 1, 0, nz - 1, lambda s: give_z(s).start())
        at(i, 0, nz, restore)
        at(i - lag_core, 0, nz, over_cores)
        at(i - lag_mesh, 0, nz, over_mesh)

    each(0, nz + lag_mesh + 1, third_phase)

    def relay(b):
        k = lax.rem(b, share)
        return remote(z_in.at[slab(b)], relay_in.at[slab(k)], rr_s.at[k], rr_r.at[k], y_peer)

    def store(k, own):
        src = z_in.at[slab(m * share + k)] if own else relay_in.at[slab(k)]
        j = m if own else other_m
        return pltpu.make_async_copy(src, applied.at[plane(k, j)], out_s.at[0 if own else 1, k])

    def overlap(k, j, values, fresh):
        other = turned(values)
        sums = []
        for factor in (values, other):
            for a in range(nbands):
                sums.append(jnp.sum(mine[plane(a, j), :] * factor, axis=0, keepdims=True))
        total = jnp.concatenate(sums, 0)
        acc[k] = total if fresh else acc[k] + total

    def settle(b):
        owner, k = lax.div(b, share), lax.rem(b, share)

        def own():
            store(k, True).start()
            overlap(k, m, z_in[slab(b), :], True)

        pl.when(owner == m)(own)
        pl.when(owner != m)(lambda: relay(b).start())

    def relayed(b):
        def own():
            k = lax.rem(b, share)
            relay(other_m * share + k).wait_recv()
            store(k, False).start()
            overlap(k, other_m, relay_in[slab(k), :], False)

        pl.when(lax.div(b, share) == m)(own)

    def arrive(i):
        pl.when(i > 0)(lambda: give_z_in(i - 1).wait_recv())
        pl.when(i < nz)(lambda: settle(source(jnp.where(i == 0, nz - 1, i - 1))))

    lag_relay = 2

    def arrive_step(i):
        pl.when(i < nz)(lambda: arrive(i))
        before = i - lag_relay
        pl.when(before >= 0)(
            lambda: relayed(source(jnp.where(before == 0, nz - 1, before - 1)))
        )

    each(0, nz + lag_relay, arrive_step)

    tile = jnp.zeros((block, 128), F32)
    tile_lane = lax.broadcasted_iota(jnp.int32, (block, 128), 1)
    for k in range(share):
        rows_of = acc[k]
        for group in range(4):
            column_sum = jnp.sum(
                rows_of[group * block : (group + 1) * block], axis=1, keepdims=True
            )
            here = tile_lane == group * nbands + share * m + k
            tile = tile + jnp.where(here, column_sum, 0.0)
    pz[z] = tile * (1.0 / float(points**3))

    def sum_z(i):
        return remote(pz.at[z], pz.at[z], ib_s.at[i], ib_r.at[i], ring(target(i)))

    def sum_z_in(i):
        spot = pz.at[source(i)]
        return remote(spot, spot, ib_s.at[i], ib_r.at[i], ring(source(i)))

    each(0, steps, lambda i: sum_z(steps - 1 - i).start())
    each(0, steps, lambda i: sum_z_in(i).wait_recv())
    whole = pz[0]
    for k in range(1, nz):
        whole = whole + pz[k]
    quarter = 2 * m + c
    fin[quarter] = whole
    peers = [
        (core_peer, 2 * m + other_c),
        (y_peer, 2 * other_m + c),
        (diag_peer, 2 * other_m + other_c),
    ]

    def spread(k, into):
        spot = fin.at[into]
        return remote(spot, spot, ic_s.at[k], ic_r.at[k], peers[k][0])

    for k in range(3):
        spread(k, quarter).start()
    for k in range(3):
        spread(k, peers[k][1]).wait_recv()
    result = (fin[0] + fin[1]) + (fin[2] + fin[3])
    for group in range(4):
        turned_tile = result if group == 0 else pltpu.roll(result, 128 - group * nbands, 1)
        inter[group * block : (group + 1) * block, :] = turned_tile[:, :nbands]

    for k in range(1, far_count):
        occ_far_z(k).wait_send()
    for k in range(near_count - 1):
        occ_near_z(k).wait_send()
    each(0, steps, lambda i: band_z(i).wait_send())
    band_own(False).wait_send()
    occ_far(path).wait_send()
    for j in range(1, nx):
        occ_x(j, 0, path).wait_send()
        occ_x(j, 1, far_path).wait_send()
    each(0, npath, lambda p: occ_core(c, p).wait_send())
    each(0, steps, lambda i: band_y(i, m).wait_send())
    each(0, steps, lambda i: band_core(i, c, m, 0).wait_send())
    each(0, steps, lambda i: band_core(i, c, other_m, 1).wait_send())
    each(0, nz, lambda i: give_core(i).wait_send())
    each(0, nz, lambda i: give_y(i).wait_send())
    each(0, steps, lambda i: give_z(i).wait_send())
    each(0, share, lambda k: relay(other_m * share + k).wait_send())
    each(0, share, lambda k: store(k, True).wait())
    each(0, share, lambda k: store(k, False).wait())
    for k in range(3):
        spread(k, quarter).wait_send()
    each(0, steps, lambda i: sum_z(i).wait_send())


def per_device(path_bands, occupied, path_kpts, mesh_kpts, mesh_shift):
    nbands, planes, points, width = path_bands.shape[1:]
    npath = lax.axis_size("path")
    nz = lax.axis_size("grid") // 2
    assert planes == 2 and nz == nbands and lax.axis_size("mesh") == 2
    half = points // 2
    share = nbands // 2
    forward_y, along_x, inverse_y, forward_z, inverse_z = tables(points)
    far_count, near_count, pitch = layout(points, nz)
    in_hbm = lambda array: pltpu.with_memory_space_constraint(array, pltpu.HBM)
    anywhere = pl.BlockSpec(memory_space=pl.ANY)
    vmem = lambda *shape: pltpu.VMEM(shape, F32)
    table = lambda array: pltpu.VMEM(array.shape, BF16)
    dma = lambda *shape: pltpu.SemaphoreType.DMA(shape)
    block = 2 * nbands // 4
    pairs = lambda *shape: [dma(*shape), dma(*shape)]
    scratch = [
        vmem(nz, 2, 2, points, width),
        vmem(far_count, near_count, 2, 2, points, width),
        vmem(points * pitch, width),
        vmem(nz, 2, 2, points, width),
        vmem(nz, 2, points, width),
        vmem(nz, points, width),
        vmem(nz, points, width),
        vmem(nz, points, width),
        vmem(nbands * points, width),
        vmem(share * points, width),
        vmem(nbands * 2 * points, width),
        table(forward_y[0]),
        table(along_x),
        table(inverse_y[0]),
        table(forward_z),
        table(inverse_z),
        vmem(points, width),
        vmem(share, 2 * nbands, width),
        vmem(nz, block, 128),
        vmem(4, block, 128),
        pltpu.SMEM(path_kpts.shape, jnp.int32),
        pltpu.SMEM(mesh_kpts.shape, jnp.int32),
        pltpu.SMEM(mesh_shift.shape, jnp.int32),
        dma(12),
        *pairs(far_count),
        *pairs(near_count),
        *pairs(1),
        *pairs(2, max(npath // 2, 1)),
        *pairs(npath),
        *pairs(nz),
        *pairs(nz),
        *pairs(2, nz),
        *pairs(1),
        *pairs(nz),
        *pairs(nz),
        *pairs(nz),
        *pairs(share),
        dma(2, share),
        *pairs(nz),
        *pairs(3),
    ]
    applied, inter = pl.pallas_call(
        functools.partial(body, points, nz, npath, nbands),
        name="exchange",
        out_shape=(
            jax.ShapeDtypeStruct((share * 2 * points, width), F32),
            jax.ShapeDtypeStruct((2 * nbands, nbands), F32),
        ),
        in_specs=[anywhere] * 10,
        out_specs=(anywhere, pl.BlockSpec(memory_space=pltpu.VMEM)),
        scratch_shapes=scratch,
        compiler_params=pltpu.CompilerParams(
            collective_id=0, has_side_effects=True, vmem_limit_bytes=40 << 20
        ),
    )(
        *map(
            in_hbm,
            (
                path_kpts,
                mesh_kpts,
                mesh_shift,
                path_bands.reshape(nbands * planes * points, width),
                occupied,
                jnp.asarray(forward_y),
                jnp.asarray(along_x),
                jnp.asarray(inverse_y),
                jnp.asarray(forward_z),
                jnp.asarray(inverse_z),
            ),
        )
    )
    return (
        applied.reshape(1, share, planes, points, width),
        inter.reshape(1, 2, nbands, nbands),
    )


def solution(mesh):
    return jax.shard_map(
        per_device,
        mesh=mesh,
        in_specs=(
            P("path", None, "grid", None, None),
            P("mesh", None, "grid", "path", None),
            P("path", None),
            P(),
            P(),
        ),
        out_specs=(P("path", "mesh", "grid", None, None), P("path", None, None, None)),
        check_vma=False,
    )
```

```python
import functools
import math

import jax
import jax.numpy as jnp
import ml_dtypes
import numpy as np
from jax import lax
from jax.experimental import pallas as pl
from jax.experimental.pallas import tpu as pltpu
from jax.sharding import PartitionSpec as P

KDIV = 8
BOX_LENGTH = 42.7
SCREEN_SQ = 0.04
MIXING = 0.25
MESH = pl.DeviceIdType.MESH
F32 = jnp.float32
BF16 = jnp.bfloat16


def two_terms(table):
    high = table.astype(ml_dtypes.bfloat16)
    low = (table - high.astype(np.float64)).astype(ml_dtypes.bfloat16)
    return high, low


def tables(points):
    half = points // 2
    grid = np.arange(points)
    angles = 2.0 * np.pi / points * (grid[:, None] * grid[None, :] % points)
    cosine, sine = np.cos(angles), np.sin(angles)

    def left(cos_part, sin_part):
        high, low = two_terms(np.concatenate([cos_part, sin_part], 0))
        return np.concatenate([high, high, low, low], 1)

    def right(matrix):
        high, low = two_terms(matrix)
        upper = np.concatenate([high, low], 1)
        lower = np.concatenate([high, np.zeros_like(low)], 1)
        return np.concatenate([upper, lower], 0)

    parts = [slice(0, half), slice(half, points)]
    forward_y = np.stack([left(cosine[part], sine[part]) for part in parts])
    inverse_y = np.stack([left(cosine[:, part], sine[:, part]) for part in parts])
    along_x = left(cosine, sine)
    forward_z = right(np.block([[cosine, -sine], [sine, cosine]]))
    inverse_z = right(np.block([[cosine, sine], [-sine, cosine]]))
    return forward_y, along_x, inverse_y, forward_z, inverse_z


def split(values):
    high = values.astype(BF16)
    return high, (values - high.astype(F32)).astype(BF16)


def layout(points, nz):
    near_count = {16: 4}.get(nz, 2)
    return nz // near_count, near_count, points // 2 + 8


def body(
    points, nz, npath, nbands,
    kp_h, km_h, shift_h, bands, occ, fy_h, lx_h, iy_h, fz_h, iz_h,
    applied, inter,
    band_full, occ_full, field, part, core_in, y_out, y_in, z_out, z_in, relay_in, mine,
    fy, lx, iy, fz, iz, base, acc, pz, fin, kp, km, shift,
    loc, on_s, on_r, oh_s, oh_r, ox_s, ox_r, oc_s, oc_r,
    bz_s, bz_r, by_s, by_r, bc_s, bc_r, bl_s, bl_r,
    rc_s, rc_r, ry_s, ry_r, rz_s, rz_r, rr_s, rr_r, out_s,
    ib_s, ib_r, ic_s, ic_r,
):
    width = 2 * points
    half = points // 2
    nx = npath // 2
    rows = points // npath
    share = nbands // 2
    block = nbands // 2
    far_count, near_count, pitch = layout(points, nz)

    path = lax.axis_index("path")
    m = lax.axis_index("mesh")
    g = lax.axis_index("grid")
    z = lax.div(g, 2)
    c = lax.rem(g, 2)
    hi_y = lax.div(path, nx)
    at_x = lax.rem(path, nx)
    other_c, other_m = 1 - c, 1 - m
    core_peer = {"grid": 2 * z + other_c}
    y_peer = {"mesh": other_m}
    diag_peer = {"mesh": other_m, "grid": 2 * z + other_c}
    far_path = (1 - hi_y) * nx + at_x
    far_peer = {"path": far_path}

    def x_peer(j):
        return hi_y * nx + lax.rem(at_x + j, nx)

    def offset(i):
        return (lax.div(i, 2) + 1) * (1 - 2 * lax.rem(i, 2)) * jnp.where(i == nz - 1, 0, 1)

    def target(i):
        return lax.rem(z + offset(i) + nz, nz)

    def source(i):
        return lax.rem(z - offset(i) + nz, nz)

    def ring(zz):
        return {"grid": 2 * zz + c}

    def remote(src, dst, send, recv, peer):
        return pltpu.make_async_remote_copy(
            src_ref=src, dst_ref=dst, send_sem=send, recv_sem=recv, device_id=peer, device_id_type=MESH
        )

    def plane(b, j):
        return pl.ds(pl.multiple_of((b * 2 + j) * points, points), points)

    def slab(b):
        return pl.ds(pl.multiple_of(b * points, points), points)

    def path_rows(p):
        return pl.ds(pl.multiple_of(p * rows, rows), rows)

    my_rows = path_rows(path)
    far, near = lax.div(z, near_count), lax.rem(z, near_count)
    local = [
        pltpu.make_async_copy(occ.at[0, 0], occ_full.at[far, near, c, :, my_rows, :], loc.at[0]),
        pltpu.make_async_copy(bands.at[plane(z, 0)], band_full.at[z, c, 0], loc.at[1]),
        pltpu.make_async_copy(bands.at[plane(z, 1)], band_full.at[z, c, 1], loc.at[2]),
        pltpu.make_async_copy(fy_h.at[c], fy, loc.at[3]),
        pltpu.make_async_copy(lx_h, lx, loc.at[4]),
        pltpu.make_async_copy(iy_h.at[c], iy, loc.at[5]),
        pltpu.make_async_copy(fz_h, fz, loc.at[6]),
        pltpu.make_async_copy(iz_h, iz, loc.at[7]),
        pltpu.make_async_copy(kp_h, kp, loc.at[8]),
        pltpu.make_async_copy(km_h, km, loc.at[9]),
        pltpu.make_async_copy(shift_h, shift, loc.at[10]),
        pltpu.make_async_copy(bands, mine, loc.at[11]),
    ]
    for copy in local:
        copy.start()

    barrier = pltpu.get_barrier_semaphore()

    def greet(i, carry):
        pl.semaphore_signal(barrier, inc=1, device_id=ring(target(i)), device_id_type=MESH)
        return carry

    lax.fori_loop(0, nz - 1, greet, 0)
    for peer in (core_peer, y_peer, diag_peer, far_peer):
        pl.semaphore_signal(barrier, inc=1, device_id=peer, device_id_type=MESH)
    for j in range(1, nx):
        pl.semaphore_signal(barrier, inc=1, device_id={"path": x_peer(j)}, device_id_type=MESH)

    pl.semaphore_wait(barrier, nz - 1 + 4 + nx - 1)

    def each(low, high, action):
        def step(i, carry):
            action(i)
            return carry

        lax.fori_loop(low, high, step, 0)

    def occ_z(i, back=False):
        zz = source(i) if back else z
        spot = occ_full.at[lax.div(zz, near_count), lax.rem(zz, near_count), c, :, my_rows, :]
        src = spot if back else occ.at[0, 0]
        return remote(src, spot, on_s.at[i], on_r.at[i], ring(source(i) if back else target(i)))

    def band_z(i):
        dz = target(i)
        return remote(
            bands.at[plane(dz, m)], band_full.at[z, c, m], bz_s.at[i], bz_r.at[i], ring(dz)
        )

    def band_z_in(i):
        spot = band_full.at[source(i), c, m]
        return remote(spot, spot, bz_s.at[i], bz_r.at[i], ring(source(i)))

    def band_own(to_mine):
        spot = band_full.at[z, other_c if to_mine else c]
        return remote(spot, spot, bl_s.at[0], bl_r.at[0], core_peer)

    def column(cc, p):
        return occ_full.at[:, :, cc, :, path_rows(p), :]

    def occ_far(p):
        return remote(column(c, p), column(c, p), oh_s.at[0], oh_r.at[0], far_peer)

    def occ_x(j, which, p):
        spot = column(c, p)
        return remote(
            spot, spot, ox_s.at[which, j], ox_r.at[which, j], {"path": x_peer(j)}
        )

    def occ_core(cc, p):
        spot = column(cc, p)
        return remote(spot, spot, oc_s.at[p], oc_r.at[p], core_peer)

    def band_y(i, j):
        spot = band_full.at[source(i), c, j]
        return remote(spot, spot, by_s.at[i], by_r.at[i], y_peer)

    def band_core(i, cc, j, which):
        spot = band_full.at[source(i), cc, j]
        return remote(spot, spot, bc_s.at[which, i], bc_r.at[which, i], core_peer)

    def late(i):
        band_y(i, other_m).wait_recv()
        band_core(i, c, other_m, 1).start()

    def forward(i):
        band_z_in(i).wait_recv()
        band_y(i, m).start()
        band_core(i, c, m, 0).start()

    def forward_and_late(i):
        forward(i)
        pl.when(i >= lag_y)(lambda: late(i - lag_y))

    steps = nz - 1
    lag_y = 5 if nz == 16 else 1
    first_stop, third_stop, fourth_stop = (4, 6, 10) if nz == 16 else (1, steps, steps)
    each(0, steps, lambda i: occ_z(steps - 1 - i).start())
    each(0, steps, lambda i: band_z(i).start())
    for copy in local[:3]:
        copy.wait()
    band_own(False).start()
    each(0, first_stop, forward_and_late)
    for copy in local[3:]:
        copy.wait()

    scale = (2.0 * math.pi / BOX_LENGTH) ** 2
    lane = lax.broadcasted_iota(jnp.int32, (points, width), 1)
    row = lax.broadcasted_iota(jnp.int32, (points, width), 0)

    def frequency(index, dim):
        shifted = (index - shift[m, dim] + half) & (points - 1)
        offset_frac = (kp[0, dim] - km[m, dim]).astype(F32) / KDIV
        return (shifted - half).astype(F32) + offset_frac

    freq_x = frequency(row, 0)
    freq_z = frequency(lane & (points - 1), 2)
    base[...] = scale * (freq_x * freq_x + freq_z * freq_z) + SCREEN_SQ

    each(0, steps, lambda i: occ_z(i, True).wait_recv())
    occ_far(path).start()
    for j in range(1, nx):
        occ_x(j, 0, path).start()
    occ_core(c, path).start()
    each(first_stop, third_stop, forward_and_late)
    occ_far(far_path).wait_recv()
    for j in range(1, nx):
        occ_x(j, 1, far_path).start()
    occ_core(c, far_path).start()
    each(third_stop, fourth_stop, forward_and_late)
    for which in range(2):
        for j in range(1, nx):
            side = hi_y if which == 0 else 1 - hi_y
            p = side * nx + lax.rem(at_x - j + nx, nx)
            occ_x(j, which, p).wait_recv()
            occ_core(c, p).start()
    each(0, npath, lambda p: occ_core(other_c, p).wait_recv())

    lanes = lax.broadcasted_iota(jnp.int32, (1, width), 1)
    first = lanes < points

    def swap(values):
        return pltpu.roll(values, points, 1)

    def turned(values):
        moved = swap(values)
        return jnp.where(first, moved, -moved)

    def factors(values):
        moved = swap(values)
        return jnp.where(first, values, moved), jnp.where(first, moved, -values)

    def contract(matrix, tiles):
        stacked = jnp.concatenate(tiles, 1) if len(tiles) > 1 else tiles[0]
        high, low = split(stacked)
        right = jnp.concatenate([high, low, high, low], 0)
        out = jnp.dot(matrix, right, preferred_element_type=F32)
        count = out.shape[0] // 2
        return [
            (out[:count, t * width : (t + 1) * width], out[count:, t * width : (t + 1) * width])
            for t in range(len(tiles))
        ]

    def forward_sum(pair):
        return pair[0] + turned(pair[1])

    def inverse_sum(pair):
        return pair[0] - turned(pair[1])

    def along_z(matrix, values):
        high, low = split(values)
        out = jnp.dot(jnp.concatenate([high, low], 1), matrix, preferred_element_type=F32)
        return out[:, :width] + out[:, width:]

    def orbital(zz, cc, j):
        return occ_full[lax.div(zz, near_count), lax.rem(zz, near_count), cc, j]

    def x_rows(zz, t):
        return pl.ds(pl.multiple_of((zz * 4 + t) * pitch, 8), half)

    def transform(zz):
        tiles = []
        for t in range(4):
            band = band_full[zz, t // 2, t % 2]
            even, odd = factors(orbital(zz, t // 2, t % 2))
            tiles.append(even * band + odd * swap(band))
        summed = [forward_sum(pair) for pair in contract(fy[...], tiles)]
        values = along_z(fz[...], jnp.concatenate(summed, 0))
        for t in range(4):
            field[x_rows(zz, t), :] = values[t * half : (t + 1) * half]

    def first_phase(t):
        step = fourth_stop + lax.div(t, 3)
        turn = lax.rem(t, 3) == 0
        pl.when(turn & (step < steps))(lambda: forward(step))
        pl.when((t >= fourth_stop - lag_y) & (t < steps))(lambda: late(t))

        def fetched():
            band_core(t - 1, other_c, m, 0).wait_recv()
            band_core(t - 1, other_c, other_m, 1).wait_recv()

        pl.when(t > 0)(fetched)
        pl.when(t == 0)(lambda: band_own(True).wait_recv())
        transform(source(jnp.where(t == 0, nz - 1, t - 1)))

    each(0, nz, first_phase)

    batch = min(8, half)

    def second_phase(t):
        spots, tiles, kernels = [], [], []
        for k in range(batch):
            gy = t * batch + k
            spots.append(pl.ds(gy, points, stride=pitch))
            tiles.append(field[spots[k], :])
            freq_y = frequency(c * half + gy, 1)
            kernels.append(
                (-MIXING * 4.0 * math.pi / float(points**3)) / (base[...] + scale * (freq_y * freq_y))
            )
        spectra = [
            forward_sum(pair) * kernel for pair, kernel in zip(contract(lx[...], tiles), kernels)
        ]
        for k, pair in enumerate(contract(lx[...], spectra)):
            field[spots[k], :] = inverse_sum(pair)

    each(0, half // batch, second_phase)

    def offset_back(i):
        return (nz // 2 - lax.div(i + 1, 2)) * (2 * lax.rem(i, 2) - 1)

    def target_back(i):
        return lax.rem(z + offset_back(i) + nz, nz)

    def source_back(i):
        return lax.rem(z - offset_back(i) + nz, nz)

    def restore(i):
        zz = target_back(i)
        values = along_z(
            iz[...], jnp.concatenate([field[x_rows(zz, t), :] for t in range(4)], 0)
        )
        tiles = [values[t * half : (t + 1) * half] for t in range(4)]
        for t, pair in enumerate(contract(iy[...], tiles)):
            potential = inverse_sum(pair)
            even, odd = factors(orbital(zz, t // 2, t % 2))
            part[i, t // 2, t % 2] = even * potential - odd * swap(potential)

    def give_core(i):
        return remote(part.at[i, other_c], core_in.at[i], rc_s.at[i], rc_r.at[i], core_peer)

    def give_y(i):
        return remote(y_out.at[i], y_in.at[i], ry_s.at[i], ry_r.at[i], y_peer)

    def give_z(i):
        return remote(z_out.at[i], z_in.at[slab(z)], rz_s.at[i], rz_r.at[i], ring(target_back(i)))

    def give_z_in(i):
        spot = z_in.at[slab(source_back(i))]
        return remote(spot, spot, rz_s.at[i], rz_r.at[i], ring(source_back(i)))

    def over_cores(i):
        give_core(i).wait_recv()
        y_out[i] = part[i, c, other_m] + core_in[i, other_m]
        z_out[i] = part[i, c, m] + core_in[i, m]

    def over_mesh(i):
        give_y(i).wait_recv()
        total = z_out[i] + y_in[i]
        z_out[i] = total
        pl.when(i == nz - 1)(lambda: keep(total))

    def keep(total):
        z_in[slab(z), :] = total

    lag_core, lag_mesh = 2, 5

    def third_phase(i):
        def at(step, low, high, action):
            pl.when((step >= low) & (step < high))(lambda: action(step))

        at(i - 1, 0, nz, lambda s: give_core(s).start())
        at(i - lag_core - 1, 0, nz, lambda s: give_y(s).start())
        at(i - lag_mesh - 1, 0, nz - 1, lambda s: give_z(s).start())
        at(i, 0, nz, restore)
        at(i - lag_core, 0, nz, over_cores)
        at(i - lag_mesh, 0, nz, over_mesh)

    each(0, nz + lag_mesh + 1, third_phase)

    def relay(b):
        k = lax.rem(b, share)
        return remote(z_in.at[slab(b)], relay_in.at[slab(k)], rr_s.at[k], rr_r.at[k], y_peer)

    def store(k, own):
        src = z_in.at[slab(m * share + k)] if own else relay_in.at[slab(k)]
        j = m if own else other_m
        return pltpu.make_async_copy(src, applied.at[plane(k, j)], out_s.at[0 if own else 1, k])

    def overlap(k, j, values, fresh):
        other = turned(values)
        sums = []
        for factor in (values, other):
            for a in range(nbands):
                sums.append(jnp.sum(mine[plane(a, j), :] * factor, axis=0, keepdims=True))
        total = jnp.concatenate(sums, 0)
        acc[k] = total if fresh else acc[k] + total

    def settle(b):
        owner, k = lax.div(b, share), lax.rem(b, share)

        def own():
            store(k, True).start()
            overlap(k, m, z_in[slab(b), :], True)

        pl.when(owner == m)(own)
        pl.when(owner != m)(lambda: relay(b).start())

    def relayed(b):
        def own():
            k = lax.rem(b, share)
            relay(other_m * share + k).wait_recv()
            store(k, False).start()
            overlap(k, other_m, relay_in[slab(k), :], False)

        pl.when(lax.div(b, share) == m)(own)

    def arrive(i):
        pl.when(i > 0)(lambda: give_z_in(i - 1).wait_recv())
        pl.when(i < nz)(lambda: settle(source_back(jnp.where(i == 0, nz - 1, i - 1))))

    lag_relay = 5 if nz == 16 else 2

    def arrive_step(i):
        pl.when(i < nz)(lambda: arrive(i))
        before = i - lag_relay
        pl.when(before >= 0)(
            lambda: relayed(source_back(jnp.where(before == 0, nz - 1, before - 1)))
        )

    each(0, nz + lag_relay, arrive_step)

    tile = jnp.zeros((block, 128), F32)
    tile_lane = lax.broadcasted_iota(jnp.int32, (block, 128), 1)
    for k in range(share):
        rows_of = acc[k]
        for group in range(4):
            column_sum = jnp.sum(
                rows_of[group * block : (group + 1) * block], axis=1, keepdims=True
            )
            here = tile_lane == group * nbands + share * m + k
            tile = tile + jnp.where(here, column_sum, 0.0)
    pz[z] = tile * (1.0 / float(points**3))

    def sum_z(i):
        return remote(pz.at[z], pz.at[z], ib_s.at[i], ib_r.at[i], ring(target(i)))

    def sum_z_in(i):
        spot = pz.at[source(i)]
        return remote(spot, spot, ib_s.at[i], ib_r.at[i], ring(source(i)))

    each(0, steps, lambda i: sum_z(steps - 1 - i).start())
    each(0, steps, lambda i: sum_z_in(i).wait_recv())
    whole = pz[0]
    for k in range(1, nz):
        whole = whole + pz[k]
    quarter = 2 * m + c
    fin[quarter] = whole
    peers = [
        (core_peer, 2 * m + other_c),
        (y_peer, 2 * other_m + c),
        (diag_peer, 2 * other_m + other_c),
    ]

    def spread(k, into):
        spot = fin.at[into]
        return remote(spot, spot, ic_s.at[k], ic_r.at[k], peers[k][0])

    for k in range(3):
        spread(k, quarter).start()
    for k in range(3):
        spread(k, peers[k][1]).wait_recv()
    result = (fin[0] + fin[1]) + (fin[2] + fin[3])
    for group in range(4):
        turned_tile = result if group == 0 else pltpu.roll(result, 128 - group * nbands, 1)
        inter[group * block : (group + 1) * block, :] = turned_tile[:, :nbands]

    each(0, steps, lambda i: occ_z(i).wait_send())
    each(0, steps, lambda i: band_z(i).wait_send())
    band_own(False).wait_send()
    occ_far(path).wait_send()
    for j in range(1, nx):
        occ_x(j, 0, path).wait_send()
        occ_x(j, 1, far_path).wait_send()
    each(0, npath, lambda p: occ_core(c, p).wait_send())
    each(0, steps, lambda i: band_y(i, m).wait_send())
    each(0, steps, lambda i: band_core(i, c, m, 0).wait_send())
    each(0, steps, lambda i: band_core(i, c, other_m, 1).wait_send())
    each(0, nz, lambda i: give_core(i).wait_send())
    each(0, nz, lambda i: give_y(i).wait_send())
    each(0, steps, lambda i: give_z(i).wait_send())
    each(0, share, lambda k: relay(other_m * share + k).wait_send())
    each(0, share, lambda k: store(k, True).wait())
    each(0, share, lambda k: store(k, False).wait())
    for k in range(3):
        spread(k, quarter).wait_send()
    each(0, steps, lambda i: sum_z(i).wait_send())


def per_device(path_bands, occupied, path_kpts, mesh_kpts, mesh_shift):
    nbands, planes, points, width = path_bands.shape[1:]
    npath = lax.axis_size("path")
    nz = lax.axis_size("grid") // 2
    assert planes == 2 and nz == nbands and lax.axis_size("mesh") == 2
    half = points // 2
    share = nbands // 2
    forward_y, along_x, inverse_y, forward_z, inverse_z = tables(points)
    far_count, near_count, pitch = layout(points, nz)
    in_hbm = lambda array: pltpu.with_memory_space_constraint(array, pltpu.HBM)
    anywhere = pl.BlockSpec(memory_space=pl.ANY)
    vmem = lambda *shape: pltpu.VMEM(shape, F32)
    table = lambda array: pltpu.VMEM(array.shape, BF16)
    dma = lambda *shape: pltpu.SemaphoreType.DMA(shape)
    block = 2 * nbands // 4
    pairs = lambda *shape: [dma(*shape), dma(*shape)]
    scratch = [
        vmem(nz, 2, 2, points, width),
        vmem(far_count, near_count, 2, 2, points, width),
        vmem(points * pitch, width),
        vmem(nz, 2, 2, points, width),
        vmem(nz, 2, points, width),
        vmem(nz, points, width),
        vmem(nz, points, width),
        vmem(nz, points, width),
        vmem(nbands * points, width),
        vmem(share * points, width),
        vmem(nbands * 2 * points, width),
        table(forward_y[0]),
        table(along_x),
        table(inverse_y[0]),
        table(forward_z),
        table(inverse_z),
        vmem(points, width),
        vmem(share, 2 * nbands, width),
        vmem(nz, block, 128),
        vmem(4, block, 128),
        pltpu.SMEM(path_kpts.shape, jnp.int32),
        pltpu.SMEM(mesh_kpts.shape, jnp.int32),
        pltpu.SMEM(mesh_shift.shape, jnp.int32),
        dma(12),
        *pairs(nz),
        *pairs(1),
        *pairs(2, max(npath // 2, 1)),
        *pairs(npath),
        *pairs(nz),
        *pairs(nz),
        *pairs(2, nz),
        *pairs(1),
        *pairs(nz),
        *pairs(nz),
        *pairs(nz),
        *pairs(share),
        dma(2, share),
        *pairs(nz),
        *pairs(3),
    ]
    applied, inter = pl.pallas_call(
        functools.partial(body, points, nz, npath, nbands),
        name="exchange",
        out_shape=(
            jax.ShapeDtypeStruct((share * 2 * points, width), F32),
            jax.ShapeDtypeStruct((2 * nbands, nbands), F32),
        ),
        in_specs=[anywhere] * 10,
        out_specs=(anywhere, pl.BlockSpec(memory_space=pltpu.VMEM)),
        scratch_shapes=scratch,
        compiler_params=pltpu.CompilerParams(
            collective_id=0, has_side_effects=True, vmem_limit_bytes=40 << 20
        ),
    )(
        *map(
            in_hbm,
            (
                path_kpts,
                mesh_kpts,
                mesh_shift,
                path_bands.reshape(nbands * planes * points, width),
                occupied,
                jnp.asarray(forward_y),
                jnp.asarray(along_x),
                jnp.asarray(inverse_y),
                jnp.asarray(forward_z),
                jnp.asarray(inverse_z),
            ),
        )
    )
    return (
        applied.reshape(1, share, planes, points, width),
        inter.reshape(1, 2, nbands, nbands),
    )


def solution(mesh):
    return jax.shard_map(
        per_device,
        mesh=mesh,
        in_specs=(
            P("path", None, "grid", None, None),
            P("mesh", None, "grid", "path", None),
            P("path", None),
            P(),
            P(),
        ),
        out_specs=(P("path", "mesh", "grid", None, None), P("path", None, None, None)),
        check_vma=False,
    )
```

```python
import functools
import math

import jax
import jax.numpy as jnp
import ml_dtypes
import numpy as np
from jax import lax
from jax.experimental import pallas as pl
from jax.experimental.pallas import tpu as pltpu
from jax.sharding import PartitionSpec as P

KDIV = 8
BOX_LENGTH = 42.7
SCREEN_SQ = 0.04
MIXING = 0.25
MESH = pl.DeviceIdType.MESH
F32 = jnp.float32
BF16 = jnp.bfloat16


def two_terms(table):
    high = table.astype(ml_dtypes.bfloat16)
    low = (table - high.astype(np.float64)).astype(ml_dtypes.bfloat16)
    return high, low


def tables(points):
    half = points // 2
    grid = np.arange(points)
    angles = 2.0 * np.pi / points * (grid[:, None] * grid[None, :] % points)
    cosine, sine = np.cos(angles), np.sin(angles)

    def left(cos_part, sin_part):
        high, low = two_terms(np.concatenate([cos_part, sin_part], 0))
        return np.concatenate([high, high, low, low], 1)

    def right(matrix):
        high, low = two_terms(matrix)
        upper = np.concatenate([high, low], 1)
        lower = np.concatenate([high, np.zeros_like(low)], 1)
        return np.concatenate([upper, lower], 0)

    parts = [slice(0, half), slice(half, points)]
    forward_y = np.stack([left(cosine[part], sine[part]) for part in parts])
    inverse_y = np.stack([left(cosine[:, part], sine[:, part]) for part in parts])
    along_x = left(cosine, sine)
    forward_z = right(np.block([[cosine, -sine], [sine, cosine]]))
    inverse_z = right(np.block([[cosine, sine], [-sine, cosine]]))
    return forward_y, along_x, inverse_y, forward_z, inverse_z


def split(values):
    high = values.astype(BF16)
    return high, (values - high.astype(F32)).astype(BF16)


def layout(points, nz):
    near_count = {16: 4}.get(nz, 2)
    return nz // near_count, near_count, points // 2 + 8


def body(
    points, nz, npath, nbands,
    kp_h, km_h, shift_h, bands, occ, fy_h, lx_h, iy_h, fz_h, iz_h,
    applied, inter,
    band_full, occ_full, field, part, core_in, y_out, y_in, z_out, z_in, relay_in, mine,
    fy, lx, iy, fz, iz, base, acc, pz, fin, kp, km, shift,
    loc, on_s, on_r, oh_s, oh_r, ox_s, ox_r, oc_s, oc_r,
    bz_s, bz_r, by_s, by_r, bc_s, bc_r, bl_s, bl_r,
    rc_s, rc_r, ry_s, ry_r, rz_s, rz_r, rr_s, rr_r, out_s,
    ib_s, ib_r, ic_s, ic_r,
):
    width = 2 * points
    half = points // 2
    nx = npath // 2
    rows = points // npath
    share = nbands // 2
    block = nbands // 2
    far_count, near_count, pitch = layout(points, nz)

    path = lax.axis_index("path")
    m = lax.axis_index("mesh")
    g = lax.axis_index("grid")
    z = lax.div(g, 2)
    c = lax.rem(g, 2)
    hi_y = lax.div(path, nx)
    at_x = lax.rem(path, nx)
    other_c, other_m = 1 - c, 1 - m
    core_peer = {"grid": 2 * z + other_c}
    y_peer = {"mesh": other_m}
    diag_peer = {"mesh": other_m, "grid": 2 * z + other_c}
    far_path = (1 - hi_y) * nx + at_x
    far_peer = {"path": far_path}

    def x_peer(j):
        return hi_y * nx + lax.rem(at_x + j, nx)

    def offset(i):
        return (lax.div(i, 2) + 1) * (1 - 2 * lax.rem(i, 2)) * jnp.where(i == nz - 1, 0, 1)

    def target(i):
        return lax.rem(z + offset(i) + nz, nz)

    def source(i):
        return lax.rem(z - offset(i) + nz, nz)

    def ring(zz):
        return {"grid": 2 * zz + c}

    def remote(src, dst, send, recv, peer):
        return pltpu.make_async_remote_copy(
            src_ref=src, dst_ref=dst, send_sem=send, recv_sem=recv, device_id=peer, device_id_type=MESH
        )

    def plane(b, j):
        return pl.ds(pl.multiple_of((b * 2 + j) * points, points), points)

    def slab(b):
        return pl.ds(pl.multiple_of(b * points, points), points)

    def path_rows(p):
        return pl.ds(pl.multiple_of(p * rows, rows), rows)

    my_rows = path_rows(path)
    far, near = lax.div(z, near_count), lax.rem(z, near_count)
    local = [
        pltpu.make_async_copy(occ.at[0, 0], occ_full.at[far, near, c, :, my_rows, :], loc.at[0]),
        pltpu.make_async_copy(bands.at[plane(z, 0)], band_full.at[z, c, 0], loc.at[1]),
        pltpu.make_async_copy(bands.at[plane(z, 1)], band_full.at[z, c, 1], loc.at[2]),
        pltpu.make_async_copy(fy_h.at[c], fy, loc.at[3]),
        pltpu.make_async_copy(lx_h, lx, loc.at[4]),
        pltpu.make_async_copy(iy_h.at[c], iy, loc.at[5]),
        pltpu.make_async_copy(fz_h, fz, loc.at[6]),
        pltpu.make_async_copy(iz_h, iz, loc.at[7]),
        pltpu.make_async_copy(kp_h, kp, loc.at[8]),
        pltpu.make_async_copy(km_h, km, loc.at[9]),
        pltpu.make_async_copy(shift_h, shift, loc.at[10]),
        pltpu.make_async_copy(bands, mine, loc.at[11]),
    ]
    for copy in local:
        copy.start()

    barrier = pltpu.get_barrier_semaphore()

    def greet(i, carry):
        pl.semaphore_signal(barrier, inc=1, device_id=ring(target(i)), device_id_type=MESH)
        return carry

    lax.fori_loop(0, nz - 1, greet, 0)
    for peer in (core_peer, y_peer, diag_peer, far_peer):
        pl.semaphore_signal(barrier, inc=1, device_id=peer, device_id_type=MESH)
    for j in range(1, nx):
        pl.semaphore_signal(barrier, inc=1, device_id={"path": x_peer(j)}, device_id_type=MESH)

    pl.semaphore_wait(barrier, nz - 1 + 4 + nx - 1)

    def each(low, high, action):
        def step(i, carry):
            action(i)
            return carry

        lax.fori_loop(low, high, step, 0)

    def occ_z(i, back=False):
        zz = source(i) if back else z
        spot = occ_full.at[lax.div(zz, near_count), lax.rem(zz, near_count), c, :, my_rows, :]
        src = spot if back else occ.at[0, 0]
        return remote(src, spot, on_s.at[i], on_r.at[i], ring(source(i) if back else target(i)))

    def band_z(i):
        dz = target(i)
        return remote(
            bands.at[plane(dz, m)], band_full.at[z, c, m], bz_s.at[i], bz_r.at[i], ring(dz)
        )

    def band_z_in(i):
        spot = band_full.at[source(i), c, m]
        return remote(spot, spot, bz_s.at[i], bz_r.at[i], ring(source(i)))

    def band_own(to_mine):
        spot = band_full.at[z, other_c if to_mine else c]
        return remote(spot, spot, bl_s.at[0], bl_r.at[0], core_peer)

    def column(cc, p):
        return occ_full.at[:, :, cc, :, path_rows(p), :]

    def occ_far(p):
        return remote(column(c, p), column(c, p), oh_s.at[0], oh_r.at[0], far_peer)

    def occ_x(j, which, p):
        spot = column(c, p)
        return remote(
            spot, spot, ox_s.at[which, j], ox_r.at[which, j], {"path": x_peer(j)}
        )

    def occ_core(cc, p):
        spot = column(cc, p)
        return remote(spot, spot, oc_s.at[p], oc_r.at[p], core_peer)

    def band_y(i, j):
        spot = band_full.at[source(i), c, j]
        return remote(spot, spot, by_s.at[i], by_r.at[i], y_peer)

    def band_core(i, cc, j, which):
        spot = band_full.at[source(i), cc, j]
        return remote(spot, spot, bc_s.at[which, i], bc_r.at[which, i], core_peer)

    def late(i):
        band_y(i, other_m).wait_recv()
        band_core(i, c, other_m, 1).start()

    def forward(i):
        band_z_in(i).wait_recv()
        band_y(i, m).start()
        band_core(i, c, m, 0).start()

    def forward_and_late(i):
        forward(i)
        pl.when(i >= lag_y)(lambda: late(i - lag_y))

    steps = nz - 1
    lag_y = 5 if nz == 16 else 1
    first_stop, third_stop, fourth_stop = (4, 6, 12) if nz == 16 else (1, steps, steps)
    each(0, steps, lambda i: occ_z(steps - 1 - i).start())
    each(0, steps, lambda i: band_z(i).start())
    for copy in local[:3]:
        copy.wait()
    band_own(False).start()
    each(0, first_stop, forward_and_late)
    for copy in local[3:]:
        copy.wait()

    scale = (2.0 * math.pi / BOX_LENGTH) ** 2
    lane = lax.broadcasted_iota(jnp.int32, (points, width), 1)
    row = lax.broadcasted_iota(jnp.int32, (points, width), 0)

    def frequency(index, dim):
        shifted = (index - shift[m, dim] + half) & (points - 1)
        offset_frac = (kp[0, dim] - km[m, dim]).astype(F32) / KDIV
        return (shifted - half).astype(F32) + offset_frac

    freq_x = frequency(row, 0)
    freq_z = frequency(lane & (points - 1), 2)
    base[...] = scale * (freq_x * freq_x + freq_z * freq_z) + SCREEN_SQ

    each(0, steps, lambda i: occ_z(i, True).wait_recv())
    occ_far(path).start()
    for j in range(1, nx):
        occ_x(j, 0, path).start()
    occ_core(c, path).start()
    each(first_stop, third_stop, forward_and_late)
    occ_far(far_path).wait_recv()
    for j in range(1, nx):
        occ_x(j, 1, far_path).start()
    occ_core(c, far_path).start()
    each(third_stop, fourth_stop, forward_and_late)
    for which in range(2):
        for j in range(1, nx):
            side = hi_y if which == 0 else 1 - hi_y
            p = side * nx + lax.rem(at_x - j + nx, nx)
            occ_x(j, which, p).wait_recv()
            occ_core(c, p).start()
    each(0, npath, lambda p: occ_core(other_c, p).wait_recv())

    lanes = lax.broadcasted_iota(jnp.int32, (1, width), 1)
    first = lanes < points

    def swap(values):
        return pltpu.roll(values, points, 1)

    def turned(values):
        moved = swap(values)
        return jnp.where(first, moved, -moved)

    def factors(values):
        moved = swap(values)
        return jnp.where(first, values, moved), jnp.where(first, moved, -values)

    def contract(matrix, tiles):
        stacked = jnp.concatenate(tiles, 1) if len(tiles) > 1 else tiles[0]
        high, low = split(stacked)
        right = jnp.concatenate([high, low, high, low], 0)
        out = jnp.dot(matrix, right, preferred_element_type=F32)
        count = out.shape[0] // 2
        return [
            (out[:count, t * width : (t + 1) * width], out[count:, t * width : (t + 1) * width])
            for t in range(len(tiles))
        ]

    def forward_sum(pair):
        return pair[0] + turned(pair[1])

    def inverse_sum(pair):
        return pair[0] - turned(pair[1])

    def along_z(matrix, values):
        high, low = split(values)
        out = jnp.dot(jnp.concatenate([high, low], 1), matrix, preferred_element_type=F32)
        return out[:, :width] + out[:, width:]

    def orbital(zz, cc, j):
        return occ_full[lax.div(zz, near_count), lax.rem(zz, near_count), cc, j]

    def x_rows(zz, t):
        return pl.ds(pl.multiple_of((zz * 4 + t) * pitch, 8), half)

    def transform(sources):
        tiles = []
        for zz in sources:
            for t in range(4):
                band = band_full[zz, t // 2, t % 2]
                even, odd = factors(orbital(zz, t // 2, t % 2))
                tiles.append(even * band + odd * swap(band))
        summed = [forward_sum(pair) for pair in contract(fy[...], tiles)]
        values = along_z(fz[...], jnp.concatenate(summed, 0))
        for t in range(4 * len(sources)):
            field[x_rows(sources[t // 4], t % 4), :] = values[t * half : (t + 1) * half]

    group = 4

    def first_phase(t):
        step = fourth_stop + t
        pl.when(step < steps)(lambda: forward(step))
        for k in range(group):
            ahead = group * t + group - 1 + k
            pl.when((ahead >= fourth_stop - lag_y) & (ahead < steps))(
                functools.partial(late, ahead)
            )

        def fetched(i):
            band_core(i, other_c, m, 0).wait_recv()
            band_core(i, other_c, other_m, 1).wait_recv()

        pl.when(t == 0)(lambda: band_own(True).wait_recv())
        pl.when(t > 0)(lambda: fetched(group * t - 1))
        for k in range(1, group):
            fetched(group * t + k - 1)
        first = source(jnp.where(t == 0, nz - 1, group * t - 1))
        transform([first] + [source(group * t + k - 1) for k in range(1, group)])

    each(0, nz // group, first_phase)

    batch = min(16, half)

    def second_phase(t):
        spots, tiles, kernels = [], [], []
        for k in range(batch):
            gy = t * batch + k
            spots.append(pl.ds(gy, points, stride=pitch))
            tiles.append(field[spots[k], :])
            freq_y = frequency(c * half + gy, 1)
            kernels.append(
                (-MIXING * 4.0 * math.pi / float(points**3)) / (base[...] + scale * (freq_y * freq_y))
            )
        spectra = [
            forward_sum(pair) * kernel for pair, kernel in zip(contract(lx[...], tiles), kernels)
        ]
        for k, pair in enumerate(contract(lx[...], spectra)):
            field[spots[k], :] = inverse_sum(pair)

    each(0, half // batch, second_phase)

    def offset_back(i):
        return (nz // 2 - lax.div(i + 1, 2)) * (2 * lax.rem(i, 2) - 1)

    def target_back(i):
        return lax.rem(z + offset_back(i) + nz, nz)

    def source_back(i):
        return lax.rem(z - offset_back(i) + nz, nz)

    def restore(i):
        zz = target_back(i)
        values = along_z(
            iz[...], jnp.concatenate([field[x_rows(zz, t), :] for t in range(4)], 0)
        )
        tiles = [values[t * half : (t + 1) * half] for t in range(4)]
        for t, pair in enumerate(contract(iy[...], tiles)):
            potential = inverse_sum(pair)
            even, odd = factors(orbital(zz, t // 2, t % 2))
            part[i, t // 2, t % 2] = even * potential - odd * swap(potential)

    def give_core(i):
        return remote(part.at[i, other_c], core_in.at[i], rc_s.at[i], rc_r.at[i], core_peer)

    def give_y(i):
        return remote(y_out.at[i], y_in.at[i], ry_s.at[i], ry_r.at[i], y_peer)

    def give_z(i):
        return remote(z_out.at[i], z_in.at[slab(z)], rz_s.at[i], rz_r.at[i], ring(target_back(i)))

    def give_z_in(i):
        spot = z_in.at[slab(source_back(i))]
        return remote(spot, spot, rz_s.at[i], rz_r.at[i], ring(source_back(i)))

    def over_cores(i):
        give_core(i).wait_recv()
        y_out[i] = part[i, c, other_m] + core_in[i, other_m]
        z_out[i] = part[i, c, m] + core_in[i, m]

    def over_mesh(i):
        give_y(i).wait_recv()
        total = z_out[i] + y_in[i]
        z_out[i] = total
        pl.when(i == nz - 1)(lambda: keep(total))

    def keep(total):
        z_in[slab(z), :] = total

    lag_core, lag_mesh = 2, 5

    def third_phase(i):
        def at(step, low, high, action):
            pl.when((step >= low) & (step < high))(lambda: action(step))

        at(i - 1, 0, nz, lambda s: give_core(s).start())
        at(i - lag_core - 1, 0, nz, lambda s: give_y(s).start())
        at(i - lag_mesh - 1, 0, nz - 1, lambda s: give_z(s).start())
        at(i, 0, nz, restore)
        at(i - lag_core, 0, nz, over_cores)
        at(i - lag_mesh, 0, nz, over_mesh)

    each(0, nz + lag_mesh + 1, third_phase)

    def relay(b):
        k = lax.rem(b, share)
        return remote(z_in.at[slab(b)], relay_in.at[slab(k)], rr_s.at[k], rr_r.at[k], y_peer)

    def store(k, own):
        src = z_in.at[slab(m * share + k)] if own else relay_in.at[slab(k)]
        j = m if own else other_m
        return pltpu.make_async_copy(src, applied.at[plane(k, j)], out_s.at[0 if own else 1, k])

    def overlap(k, j, values, fresh):
        other = turned(values)
        sums = []
        for factor in (values, other):
            for a in range(nbands):
                sums.append(jnp.sum(mine[plane(a, j), :] * factor, axis=0, keepdims=True))
        total = jnp.concatenate(sums, 0)
        acc[k] = total if fresh else acc[k] + total

    def settle(b):
        owner, k = lax.div(b, share), lax.rem(b, share)

        def own():
            store(k, True).start()
            overlap(k, m, z_in[slab(b), :], True)

        pl.when(owner == m)(own)
        pl.when(owner != m)(lambda: relay(b).start())

    def relayed(b):
        def own():
            k = lax.rem(b, share)
            relay(other_m * share + k).wait_recv()
            store(k, False).start()
            overlap(k, other_m, relay_in[slab(k), :], False)

        pl.when(lax.div(b, share) == m)(own)

    def arrive(i):
        pl.when(i > 0)(lambda: give_z_in(i - 1).wait_recv())
        pl.when(i < nz)(lambda: settle(source_back(jnp.where(i == 0, nz - 1, i - 1))))

    lag_relay = 5 if nz == 16 else 2

    def arrive_step(i):
        pl.when(i < nz)(lambda: arrive(i))
        before = i - lag_relay
        pl.when(before >= 0)(
            lambda: relayed(source_back(jnp.where(before == 0, nz - 1, before - 1)))
        )

    each(0, nz + lag_relay, arrive_step)

    tile = jnp.zeros((block, 128), F32)
    tile_lane = lax.broadcasted_iota(jnp.int32, (block, 128), 1)
    for k in range(share):
        rows_of = acc[k]
        for group in range(4):
            column_sum = jnp.sum(
                rows_of[group * block : (group + 1) * block], axis=1, keepdims=True
            )
            here = tile_lane == group * nbands + share * m + k
            tile = tile + jnp.where(here, column_sum, 0.0)
    pz[z] = tile * (1.0 / float(points**3))

    def sum_z(i):
        return remote(pz.at[z], pz.at[z], ib_s.at[i], ib_r.at[i], ring(target(i)))

    def sum_z_in(i):
        spot = pz.at[source(i)]
        return remote(spot, spot, ib_s.at[i], ib_r.at[i], ring(source(i)))

    each(0, steps, lambda i: sum_z(steps - 1 - i).start())
    each(0, steps, lambda i: sum_z_in(i).wait_recv())
    whole = pz[0]
    for k in range(1, nz):
        whole = whole + pz[k]
    quarter = 2 * m + c
    fin[quarter] = whole
    peers = [
        (core_peer, 2 * m + other_c),
        (y_peer, 2 * other_m + c),
        (diag_peer, 2 * other_m + other_c),
    ]

    def spread(k, into):
        spot = fin.at[into]
        return remote(spot, spot, ic_s.at[k], ic_r.at[k], peers[k][0])

    for k in range(3):
        spread(k, quarter).start()
    for k in range(3):
        spread(k, peers[k][1]).wait_recv()
    result = (fin[0] + fin[1]) + (fin[2] + fin[3])
    for group in range(4):
        turned_tile = result if group == 0 else pltpu.roll(result, 128 - group * nbands, 1)
        inter[group * block : (group + 1) * block, :] = turned_tile[:, :nbands]

    each(0, steps, lambda i: occ_z(i).wait_send())
    each(0, steps, lambda i: band_z(i).wait_send())
    band_own(False).wait_send()
    occ_far(path).wait_send()
    for j in range(1, nx):
        occ_x(j, 0, path).wait_send()
        occ_x(j, 1, far_path).wait_send()
    each(0, npath, lambda p: occ_core(c, p).wait_send())
    each(0, steps, lambda i: band_y(i, m).wait_send())
    each(0, steps, lambda i: band_core(i, c, m, 0).wait_send())
    each(0, steps, lambda i: band_core(i, c, other_m, 1).wait_send())
    each(0, nz, lambda i: give_core(i).wait_send())
    each(0, nz, lambda i: give_y(i).wait_send())
    each(0, steps, lambda i: give_z(i).wait_send())
    each(0, share, lambda k: relay(other_m * share + k).wait_send())
    each(0, share, lambda k: store(k, True).wait())
    each(0, share, lambda k: store(k, False).wait())
    for k in range(3):
        spread(k, quarter).wait_send()
    each(0, steps, lambda i: sum_z(i).wait_send())


def per_device(path_bands, occupied, path_kpts, mesh_kpts, mesh_shift):
    nbands, planes, points, width = path_bands.shape[1:]
    npath = lax.axis_size("path")
    nz = lax.axis_size("grid") // 2
    assert planes == 2 and nz == nbands and lax.axis_size("mesh") == 2
    half = points // 2
    share = nbands // 2
    forward_y, along_x, inverse_y, forward_z, inverse_z = tables(points)
    far_count, near_count, pitch = layout(points, nz)
    in_hbm = lambda array: pltpu.with_memory_space_constraint(array, pltpu.HBM)
    anywhere = pl.BlockSpec(memory_space=pl.ANY)
    vmem = lambda *shape: pltpu.VMEM(shape, F32)
    table = lambda array: pltpu.VMEM(array.shape, BF16)
    dma = lambda *shape: pltpu.SemaphoreType.DMA(shape)
    block = 2 * nbands // 4
    pairs = lambda *shape: [dma(*shape), dma(*shape)]
    scratch = [
        vmem(nz, 2, 2, points, width),
        vmem(far_count, near_count, 2, 2, points, width),
        vmem(points * pitch, width),
        vmem(nz, 2, 2, points, width),
        vmem(nz, 2, points, width),
        vmem(nz, points, width),
        vmem(nz, points, width),
        vmem(nz, points, width),
        vmem(nbands * points, width),
        vmem(share * points, width),
        vmem(nbands * 2 * points, width),
        table(forward_y[0]),
        table(along_x),
        table(inverse_y[0]),
        table(forward_z),
        table(inverse_z),
        vmem(points, width),
        vmem(share, 2 * nbands, width),
        vmem(nz, block, 128),
        vmem(4, block, 128),
        pltpu.SMEM(path_kpts.shape, jnp.int32),
        pltpu.SMEM(mesh_kpts.shape, jnp.int32),
        pltpu.SMEM(mesh_shift.shape, jnp.int32),
        dma(12),
        *pairs(nz),
        *pairs(1),
        *pairs(2, max(npath // 2, 1)),
        *pairs(npath),
        *pairs(nz),
        *pairs(nz),
        *pairs(2, nz),
        *pairs(1),
        *pairs(nz),
        *pairs(nz),
        *pairs(nz),
        *pairs(share),
        dma(2, share),
        *pairs(nz),
        *pairs(3),
    ]
    applied, inter = pl.pallas_call(
        functools.partial(body, points, nz, npath, nbands),
        name="exchange",
        out_shape=(
            jax.ShapeDtypeStruct((share * 2 * points, width), F32),
            jax.ShapeDtypeStruct((2 * nbands, nbands), F32),
        ),
        in_specs=[anywhere] * 10,
        out_specs=(anywhere, pl.BlockSpec(memory_space=pltpu.VMEM)),
        scratch_shapes=scratch,
        compiler_params=pltpu.CompilerParams(
            collective_id=0, has_side_effects=True, vmem_limit_bytes=40 << 20
        ),
    )(
        *map(
            in_hbm,
            (
                path_kpts,
                mesh_kpts,
                mesh_shift,
                path_bands.reshape(nbands * planes * points, width),
                occupied,
                jnp.asarray(forward_y),
                jnp.asarray(along_x),
                jnp.asarray(inverse_y),
                jnp.asarray(forward_z),
                jnp.asarray(inverse_z),
            ),
        )
    )
    return (
        applied.reshape(1, share, planes, points, width),
        inter.reshape(1, 2, nbands, nbands),
    )


def solution(mesh):
    return jax.shard_map(
        per_device,
        mesh=mesh,
        in_specs=(
            P("path", None, "grid", None, None),
            P("mesh", None, "grid", "path", None),
            P("path", None),
            P(),
            P(),
        ),
        out_specs=(P("path", "mesh", "grid", None, None), P("path", None, None, None)),
        check_vma=False,
    )
```

```python
import functools
import math

import jax
import jax.numpy as jnp
import ml_dtypes
import numpy as np
from jax import lax
from jax.experimental import pallas as pl
from jax.experimental.pallas import tpu as pltpu
from jax.sharding import PartitionSpec as P

KDIV = 8
BOX_LENGTH = 42.7
SCREEN_SQ = 0.04
MIXING = 0.25
MESH = pl.DeviceIdType.MESH
F32 = jnp.float32
BF16 = jnp.bfloat16


def two_terms(table):
    high = table.astype(ml_dtypes.bfloat16)
    low = (table - high.astype(np.float64)).astype(ml_dtypes.bfloat16)
    return high, low


def tables(points):
    half = points // 2
    grid = np.arange(points)
    angles = 2.0 * np.pi / points * (grid[:, None] * grid[None, :] % points)
    cosine, sine = np.cos(angles), np.sin(angles)

    def left(cos_part, sin_part):
        high, low = two_terms(np.concatenate([cos_part, sin_part], 0))
        return np.concatenate([high, high, low, low], 1)

    def right(matrix):
        high, low = two_terms(matrix)
        upper = np.concatenate([high, low], 1)
        lower = np.concatenate([high, np.zeros_like(low)], 1)
        return np.concatenate([upper, lower], 0)

    parts = [slice(0, half), slice(half, points)]
    forward_y = np.stack([left(cosine[part], sine[part]) for part in parts])
    inverse_y = np.stack([left(cosine[:, part], sine[:, part]) for part in parts])
    along_x = left(cosine, sine)
    forward_z = right(np.block([[cosine, -sine], [sine, cosine]]))
    inverse_z = right(np.block([[cosine, sine], [-sine, cosine]]))
    return forward_y, along_x, inverse_y, forward_z, inverse_z


def split(values):
    high = values.astype(BF16)
    return high, (values - high.astype(F32)).astype(BF16)


def layout(points, nz):
    near_count = {16: 4}.get(nz, 2)
    return nz // near_count, near_count, points // 2 + 8


def body(
    points, nz, npath, nbands,
    kp_h, km_h, shift_h, bands, occ, fy_h, lx_h, iy_h, fz_h, iz_h,
    applied, inter,
    band_full, occ_full, field, part, core_in, y_out, y_in, z_out, z_in, relay_in, mine,
    fy, lx, iy, fz, iz, base, acc, pz, fin, kp, km, shift,
    loc, on_s, on_r, oh_s, oh_r, ox_s, ox_r, oc_s, oc_r,
    bz_s, bz_r, by_s, by_r, bc_s, bc_r, bl_s, bl_r,
    rc_s, rc_r, ry_s, ry_r, rz_s, rz_r, rr_s, rr_r, out_s,
    ib_s, ib_r, ic_s, ic_r,
):
    width = 2 * points
    half = points // 2
    nx = npath // 2
    rows = points // npath
    share = nbands // 2
    block = nbands // 2
    far_count, near_count, pitch = layout(points, nz)

    path = lax.axis_index("path")
    m = lax.axis_index("mesh")
    g = lax.axis_index("grid")
    z = lax.div(g, 2)
    c = lax.rem(g, 2)
    hi_y = lax.div(path, nx)
    at_x = lax.rem(path, nx)
    other_c, other_m = 1 - c, 1 - m
    core_peer = {"grid": 2 * z + other_c}
    y_peer = {"mesh": other_m}
    diag_peer = {"mesh": other_m, "grid": 2 * z + other_c}
    far_path = (1 - hi_y) * nx + at_x
    far_peer = {"path": far_path}

    def x_peer(j):
        return hi_y * nx + lax.rem(at_x + j, nx)

    def offset(i):
        return (lax.div(i, 2) + 1) * (1 - 2 * lax.rem(i, 2)) * jnp.where(i == nz - 1, 0, 1)

    def target(i):
        return lax.rem(z + offset(i) + nz, nz)

    def source(i):
        return lax.rem(z - offset(i) + nz, nz)

    def ring(zz):
        return {"grid": 2 * zz + c}

    def remote(src, dst, send, recv, peer):
        return pltpu.make_async_remote_copy(
            src_ref=src, dst_ref=dst, send_sem=send, recv_sem=recv, device_id=peer, device_id_type=MESH
        )

    def plane(b, j):
        return pl.ds(pl.multiple_of((b * 2 + j) * points, points), points)

    def slab(b):
        return pl.ds(pl.multiple_of(b * points, points), points)

    def path_rows(p):
        return pl.ds(pl.multiple_of(p * rows, rows), rows)

    my_rows = path_rows(path)
    far, near = lax.div(z, near_count), lax.rem(z, near_count)
    local = [
        pltpu.make_async_copy(occ.at[0, 0], occ_full.at[far, near, c, :, my_rows, :], loc.at[0]),
        pltpu.make_async_copy(bands.at[plane(z, 0)], band_full.at[z, c, 0], loc.at[1]),
        pltpu.make_async_copy(bands.at[plane(z, 1)], band_full.at[z, c, 1], loc.at[2]),
        pltpu.make_async_copy(fy_h.at[c], fy, loc.at[3]),
        pltpu.make_async_copy(lx_h, lx, loc.at[4]),
        pltpu.make_async_copy(iy_h.at[c], iy, loc.at[5]),
        pltpu.make_async_copy(fz_h, fz, loc.at[6]),
        pltpu.make_async_copy(iz_h, iz, loc.at[7]),
        pltpu.make_async_copy(kp_h, kp, loc.at[8]),
        pltpu.make_async_copy(km_h, km, loc.at[9]),
        pltpu.make_async_copy(shift_h, shift, loc.at[10]),
        pltpu.make_async_copy(bands, mine, loc.at[11]),
    ]
    for copy in local:
        copy.start()

    barrier = pltpu.get_barrier_semaphore()

    def greet(i, carry):
        pl.semaphore_signal(barrier, inc=1, device_id=ring(target(i)), device_id_type=MESH)
        return carry

    lax.fori_loop(0, nz - 1, greet, 0)
    for peer in (core_peer, y_peer, diag_peer, far_peer):
        pl.semaphore_signal(barrier, inc=1, device_id=peer, device_id_type=MESH)
    for j in range(1, nx):
        pl.semaphore_signal(barrier, inc=1, device_id={"path": x_peer(j)}, device_id_type=MESH)

    pl.semaphore_wait(barrier, nz - 1 + 4 + nx - 1)

    def each(low, high, action):
        def step(i, carry):
            action(i)
            return carry

        lax.fori_loop(low, high, step, 0)

    def occ_z(i, back=False):
        zz = source(i) if back else z
        spot = occ_full.at[lax.div(zz, near_count), lax.rem(zz, near_count), c, :, my_rows, :]
        src = spot if back else occ.at[0, 0]
        return remote(src, spot, on_s.at[i], on_r.at[i], ring(source(i) if back else target(i)))

    def band_z(i):
        dz = target(i)
        return remote(
            bands.at[plane(dz, m)], band_full.at[z, c, m], bz_s.at[i], bz_r.at[i], ring(dz)
        )

    def band_z_in(i):
        spot = band_full.at[source(i), c, m]
        return remote(spot, spot, bz_s.at[i], bz_r.at[i], ring(source(i)))

    def band_own(to_mine):
        spot = band_full.at[z, other_c if to_mine else c]
        return remote(spot, spot, bl_s.at[0], bl_r.at[0], core_peer)

    def column(cc, p):
        return occ_full.at[:, :, cc, :, path_rows(p), :]

    def occ_far(p):
        return remote(column(c, p), column(c, p), oh_s.at[0], oh_r.at[0], far_peer)

    def occ_x(j, which, p):
        spot = column(c, p)
        return remote(
            spot, spot, ox_s.at[which, j], ox_r.at[which, j], {"path": x_peer(j)}
        )

    def occ_core(cc, p):
        spot = column(cc, p)
        return remote(spot, spot, oc_s.at[p], oc_r.at[p], core_peer)

    def band_y(i, j):
        spot = band_full.at[source(i), c, j]
        return remote(spot, spot, by_s.at[i], by_r.at[i], y_peer)

    def band_core(i, cc, j, which):
        spot = band_full.at[source(i), cc, j]
        return remote(spot, spot, bc_s.at[which, i], bc_r.at[which, i], core_peer)

    def late(i):
        band_y(i, other_m).wait_recv()
        band_core(i, c, other_m, 1).start()

    def forward(i):
        band_z_in(i).wait_recv()
        band_y(i, m).start()
        band_core(i, c, m, 0).start()

    def forward_and_late(i):
        forward(i)
        pl.when(i >= lag_y)(lambda: late(i - lag_y))

    steps = nz - 1
    lag_y = 5 if nz == 16 else 1
    first_stop, third_stop, fourth_stop = (2, 4, 13) if nz == 16 else (1, steps, steps)
    each(0, steps, lambda i: occ_z(steps - 1 - i).start())
    each(0, steps, lambda i: band_z(i).start())
    for copy in local[:3]:
        copy.wait()
    band_own(False).start()
    each(0, first_stop, forward_and_late)
    for copy in local[3:]:
        copy.wait()

    scale = (2.0 * math.pi / BOX_LENGTH) ** 2
    lane = lax.broadcasted_iota(jnp.int32, (points, width), 1)
    row = lax.broadcasted_iota(jnp.int32, (points, width), 0)

    def frequency(index, dim):
        shifted = (index - shift[m, dim] + half) & (points - 1)
        offset_frac = (kp[0, dim] - km[m, dim]).astype(F32) / KDIV
        return (shifted - half).astype(F32) + offset_frac

    freq_x = frequency(row, 0)
    freq_z = frequency(lane & (points - 1), 2)
    base[...] = scale * (freq_x * freq_x + freq_z * freq_z) + SCREEN_SQ

    each(0, steps, lambda i: occ_z(i, True).wait_recv())
    occ_far(path).start()
    for j in range(1, nx):
        occ_x(j, 0, path).start()
    occ_core(c, path).start()
    each(first_stop, third_stop, forward_and_late)
    occ_far(far_path).wait_recv()
    for j in range(1, nx):
        occ_x(j, 1, far_path).start()
    occ_core(c, far_path).start()
    each(third_stop, fourth_stop, forward_and_late)
    for which in range(2):
        for j in range(1, nx):
            side = hi_y if which == 0 else 1 - hi_y
            p = side * nx + lax.rem(at_x - j + nx, nx)
            occ_x(j, which, p).wait_recv()
            occ_core(c, p).start()
    each(0, npath, lambda p: occ_core(other_c, p).wait_recv())

    lanes = lax.broadcasted_iota(jnp.int32, (1, width), 1)
    first = lanes < points

    def swap(values):
        return pltpu.roll(values, points, 1)

    def turned(values):
        moved = swap(values)
        return jnp.where(first, moved, -moved)

    def factors(values):
        moved = swap(values)
        return jnp.where(first, values, moved), jnp.where(first, moved, -values)

    def contract(matrix, tiles):
        stacked = jnp.concatenate(tiles, 1) if len(tiles) > 1 else tiles[0]
        high, low = split(stacked)
        right = jnp.concatenate([high, low, high, low], 0)
        out = jnp.dot(matrix, right, preferred_element_type=F32)
        count = out.shape[0] // 2
        return [
            (out[:count, t * width : (t + 1) * width], out[count:, t * width : (t + 1) * width])
            for t in range(len(tiles))
        ]

    def forward_sum(pair):
        return pair[0] + turned(pair[1])

    def inverse_sum(pair):
        return pair[0] - turned(pair[1])

    def along_z(matrix, values):
        high, low = split(values)
        out = jnp.dot(jnp.concatenate([high, low], 1), matrix, preferred_element_type=F32)
        return out[:, :width] + out[:, width:]

    def orbital(zz, cc, j):
        return occ_full[lax.div(zz, near_count), lax.rem(zz, near_count), cc, j]

    def x_rows(zz, t):
        return pl.ds(pl.multiple_of((zz * 4 + t) * pitch, 8), half)

    def transform(sources):
        tiles = []
        for zz in sources:
            for t in range(4):
                band = band_full[zz, t // 2, t % 2]
                even, odd = factors(orbital(zz, t // 2, t % 2))
                tiles.append(even * band + odd * swap(band))
        summed = [forward_sum(pair) for pair in contract(fy[...], tiles)]
        values = along_z(fz[...], jnp.concatenate(summed, 0))
        for t in range(4 * len(sources)):
            field[x_rows(sources[t // 4], t % 4), :] = values[t * half : (t + 1) * half]

    group = 4

    def first_phase(t):
        step = fourth_stop + t
        pl.when(step < steps)(lambda: forward(step))
        for k in range(group):
            ahead = group * t + group - 1 + k
            pl.when((ahead >= fourth_stop - lag_y) & (ahead < steps))(
                functools.partial(late, ahead)
            )

        def fetched(i):
            band_core(i, other_c, m, 0).wait_recv()
            band_core(i, other_c, other_m, 1).wait_recv()

        pl.when(t == 0)(lambda: band_own(True).wait_recv())
        pl.when(t > 0)(lambda: fetched(group * t - 1))
        for k in range(1, group):
            fetched(group * t + k - 1)
        first = source(jnp.where(t == 0, nz - 1, group * t - 1))
        transform([first] + [source(group * t + k - 1) for k in range(1, group)])

    each(0, nz // group, first_phase)

    batch = min(16, half)

    def second_phase(t):
        spots, tiles, kernels = [], [], []
        for k in range(batch):
            gy = t * batch + k
            spots.append(pl.ds(gy, points, stride=pitch))
            tiles.append(field[spots[k], :])
            freq_y = frequency(c * half + gy, 1)
            kernels.append(
                (-MIXING * 4.0 * math.pi / float(points**3)) / (base[...] + scale * (freq_y * freq_y))
            )
        spectra = [
            forward_sum(pair) * kernel for pair, kernel in zip(contract(lx[...], tiles), kernels)
        ]
        for k, pair in enumerate(contract(lx[...], spectra)):
            field[spots[k], :] = inverse_sum(pair)

    each(0, half // batch, second_phase)

    def offset_back(i):
        return (nz // 2 - lax.div(i + 1, 2)) * (2 * lax.rem(i, 2) - 1)

    def target_back(i):
        return lax.rem(z + offset_back(i) + nz, nz)

    def source_back(i):
        return lax.rem(z - offset_back(i) + nz, nz)

    def restore(i):
        zz = target_back(i)
        values = along_z(
            iz[...], jnp.concatenate([field[x_rows(zz, t), :] for t in range(4)], 0)
        )
        tiles = [values[t * half : (t + 1) * half] for t in range(4)]
        for t, pair in enumerate(contract(iy[...], tiles)):
            potential = inverse_sum(pair)
            even, odd = factors(orbital(zz, t // 2, t % 2))
            part[i, t // 2, t % 2] = even * potential - odd * swap(potential)

    def give_core(i):
        return remote(part.at[i, other_c], core_in.at[i], rc_s.at[i], rc_r.at[i], core_peer)

    def give_y(i):
        return remote(y_out.at[i], y_in.at[i], ry_s.at[i], ry_r.at[i], y_peer)

    def give_z(i):
        return remote(z_out.at[i], z_in.at[slab(z)], rz_s.at[i], rz_r.at[i], ring(target_back(i)))

    def give_z_in(i):
        spot = z_in.at[slab(source_back(i))]
        return remote(spot, spot, rz_s.at[i], rz_r.at[i], ring(source_back(i)))

    def over_cores(i):
        give_core(i).wait_recv()
        y_out[i] = part[i, c, other_m] + core_in[i, other_m]
        z_out[i] = part[i, c, m] + core_in[i, m]

    def over_mesh(i):
        give_y(i).wait_recv()
        total = z_out[i] + y_in[i]
        z_out[i] = total
        pl.when(i == nz - 1)(lambda: keep(total))

    def keep(total):
        z_in[slab(z), :] = total

    lag_core, lag_mesh = 2, 5

    def third_phase(i):
        def at(step, low, high, action):
            pl.when((step >= low) & (step < high))(lambda: action(step))

        at(i - 1, 0, nz, lambda s: give_core(s).start())
        at(i - lag_core - 1, 0, nz, lambda s: give_y(s).start())
        at(i - lag_mesh - 1, 0, nz - 1, lambda s: give_z(s).start())
        at(i, 0, nz, restore)
        at(i - lag_core, 0, nz, over_cores)
        at(i - lag_mesh, 0, nz, over_mesh)

    each(0, nz + lag_mesh + 1, third_phase)

    def relay(b):
        k = lax.rem(b, share)
        return remote(z_in.at[slab(b)], relay_in.at[slab(k)], rr_s.at[k], rr_r.at[k], y_peer)

    def store(k, own):
        src = z_in.at[slab(m * share + k)] if own else relay_in.at[slab(k)]
        j = m if own else other_m
        return pltpu.make_async_copy(src, applied.at[plane(k, j)], out_s.at[0 if own else 1, k])

    def overlap(k, j, values, fresh):
        other = turned(values)
        sums = []
        for factor in (values, other):
            for a in range(nbands):
                sums.append(jnp.sum(mine[plane(a, j), :] * factor, axis=0, keepdims=True))
        total = jnp.concatenate(sums, 0)
        acc[k] = total if fresh else acc[k] + total

    def settle(b):
        owner, k = lax.div(b, share), lax.rem(b, share)

        def own():
            store(k, True).start()
            overlap(k, m, z_in[slab(b), :], True)

        pl.when(owner == m)(own)
        pl.when(owner != m)(lambda: relay(b).start())

    def relayed(b):
        def own():
            k = lax.rem(b, share)
            relay(other_m * share + k).wait_recv()
            store(k, False).start()
            overlap(k, other_m, relay_in[slab(k), :], False)

        pl.when(lax.div(b, share) == m)(own)

    def arrive(i):
        pl.when(i > 0)(lambda: give_z_in(i - 1).wait_recv())
        pl.when(i < nz)(lambda: settle(source_back(jnp.where(i == 0, nz - 1, i - 1))))

    lag_relay = 8 if nz == 16 else 2

    def arrive_step(i):
        pl.when(i < nz)(lambda: arrive(i))
        before = i - lag_relay
        pl.when(before >= 0)(
            lambda: relayed(source_back(jnp.where(before == 0, nz - 1, before - 1)))
        )

    each(0, nz + lag_relay, arrive_step)

    tile = jnp.zeros((block, 128), F32)
    tile_lane = lax.broadcasted_iota(jnp.int32, (block, 128), 1)
    for k in range(share):
        rows_of = acc[k]
        for group in range(4):
            column_sum = jnp.sum(
                rows_of[group * block : (group + 1) * block], axis=1, keepdims=True
            )
            here = tile_lane == group * nbands + share * m + k
            tile = tile + jnp.where(here, column_sum, 0.0)
    pz[z] = tile * (1.0 / float(points**3))

    def sum_z(i):
        return remote(pz.at[z], pz.at[z], ib_s.at[i], ib_r.at[i], ring(target(i)))

    def sum_z_in(i):
        spot = pz.at[source(i)]
        return remote(spot, spot, ib_s.at[i], ib_r.at[i], ring(source(i)))

    each(0, steps, lambda i: sum_z(steps - 1 - i).start())
    each(0, steps, lambda i: sum_z_in(i).wait_recv())
    whole = pz[0]
    for k in range(1, nz):
        whole = whole + pz[k]
    quarter = 2 * m + c
    fin[quarter] = whole
    peers = [
        (core_peer, 2 * m + other_c),
        (y_peer, 2 * other_m + c),
        (diag_peer, 2 * other_m + other_c),
    ]

    def spread(k, into):
        spot = fin.at[into]
        return remote(spot, spot, ic_s.at[k], ic_r.at[k], peers[k][0])

    for k in range(3):
        spread(k, quarter).start()
    for k in range(3):
        spread(k, peers[k][1]).wait_recv()
    result = (fin[0] + fin[1]) + (fin[2] + fin[3])
    for group in range(4):
        turned_tile = result if group == 0 else pltpu.roll(result, 128 - group * nbands, 1)
        inter[group * block : (group + 1) * block, :] = turned_tile[:, :nbands]

    each(0, steps, lambda i: occ_z(i).wait_send())
    each(0, steps, lambda i: band_z(i).wait_send())
    band_own(False).wait_send()
    occ_far(path).wait_send()
    for j in range(1, nx):
        occ_x(j, 0, path).wait_send()
        occ_x(j, 1, far_path).wait_send()
    each(0, npath, lambda p: occ_core(c, p).wait_send())
    each(0, steps, lambda i: band_y(i, m).wait_send())
    each(0, steps, lambda i: band_core(i, c, m, 0).wait_send())
    each(0, steps, lambda i: band_core(i, c, other_m, 1).wait_send())
    each(0, nz, lambda i: give_core(i).wait_send())
    each(0, nz, lambda i: give_y(i).wait_send())
    each(0, steps, lambda i: give_z(i).wait_send())
    each(0, share, lambda k: relay(other_m * share + k).wait_send())
    each(0, share, lambda k: store(k, True).wait())
    each(0, share, lambda k: store(k, False).wait())
    for k in range(3):
        spread(k, quarter).wait_send()
    each(0, steps, lambda i: sum_z(i).wait_send())


def per_device(path_bands, occupied, path_kpts, mesh_kpts, mesh_shift):
    nbands, planes, points, width = path_bands.shape[1:]
    npath = lax.axis_size("path")
    nz = lax.axis_size("grid") // 2
    assert planes == 2 and nz == nbands and lax.axis_size("mesh") == 2
    half = points // 2
    share = nbands // 2
    forward_y, along_x, inverse_y, forward_z, inverse_z = tables(points)
    far_count, near_count, pitch = layout(points, nz)
    in_hbm = lambda array: pltpu.with_memory_space_constraint(array, pltpu.HBM)
    anywhere = pl.BlockSpec(memory_space=pl.ANY)
    vmem = lambda *shape: pltpu.VMEM(shape, F32)
    table = lambda array: pltpu.VMEM(array.shape, BF16)
    dma = lambda *shape: pltpu.SemaphoreType.DMA(shape)
    block = 2 * nbands // 4
    pairs = lambda *shape: [dma(*shape), dma(*shape)]
    scratch = [
        vmem(nz, 2, 2, points, width),
        vmem(far_count, near_count, 2, 2, points, width),
        vmem(points * pitch, width),
        vmem(nz, 2, 2, points, width),
        vmem(nz, 2, points, width),
        vmem(nz, points, width),
        vmem(nz, points, width),
        vmem(nz, points, width),
        vmem(nbands * points, width),
        vmem(share * points, width),
        vmem(nbands * 2 * points, width),
        table(forward_y[0]),
        table(along_x),
        table(inverse_y[0]),
        table(forward_z),
        table(inverse_z),
        vmem(points, width),
        vmem(share, 2 * nbands, width),
        vmem(nz, block, 128),
        vmem(4, block, 128),
        pltpu.SMEM(path_kpts.shape, jnp.int32),
        pltpu.SMEM(mesh_kpts.shape, jnp.int32),
        pltpu.SMEM(mesh_shift.shape, jnp.int32),
        dma(12),
        *pairs(nz),
        *pairs(1),
        *pairs(2, max(npath // 2, 1)),
        *pairs(npath),
        *pairs(nz),
        *pairs(nz),
        *pairs(2, nz),
        *pairs(1),
        *pairs(nz),
        *pairs(nz),
        *pairs(nz),
        *pairs(share),
        dma(2, share),
        *pairs(nz),
        *pairs(3),
    ]
    applied, inter = pl.pallas_call(
        functools.partial(body, points, nz, npath, nbands),
        name="exchange",
        out_shape=(
            jax.ShapeDtypeStruct((share * 2 * points, width), F32),
            jax.ShapeDtypeStruct((2 * nbands, nbands), F32),
        ),
        in_specs=[anywhere] * 10,
        out_specs=(anywhere, pl.BlockSpec(memory_space=pltpu.VMEM)),
        scratch_shapes=scratch,
        compiler_params=pltpu.CompilerParams(
            collective_id=0, has_side_effects=True, vmem_limit_bytes=40 << 20
        ),
    )(
        *map(
            in_hbm,
            (
                path_kpts,
                mesh_kpts,
                mesh_shift,
                path_bands.reshape(nbands * planes * points, width),
                occupied,
                jnp.asarray(forward_y),
                jnp.asarray(along_x),
                jnp.asarray(inverse_y),
                jnp.asarray(forward_z),
                jnp.asarray(inverse_z),
            ),
        )
    )
    return (
        applied.reshape(1, share, planes, points, width),
        inter.reshape(1, 2, nbands, nbands),
    )


def solution(mesh):
    return jax.shard_map(
        per_device,
        mesh=mesh,
        in_specs=(
            P("path", None, "grid", None, None),
            P("mesh", None, "grid", "path", None),
            P("path", None),
            P(),
            P(),
        ),
        out_specs=(P("path", "mesh", "grid", None, None), P("path", None, None, None)),
        check_vma=False,
    )
```
